32 devices in a mesh: group: 2 (over y), fsdp: 16 (over z, x, core).
Axes of the slice: x: 2, y: 2, z: 4, core: 2. Of those that a mesh axis runs over, the one named last changes fastest.
Arguments:
- acts: bfloat16 [2, 8192, 8192], P('group', 'fsdp'), may hold values from -6 to 6
- cotangent: bfloat16 [2, 8192, 512], P('group', 'fsdp'), may hold values from -5.40625 to 5.40625
- inner_params: float32 [2, 8192, 512], P('group', 'fsdp'), may hold values from -6 to 6
- adam_first: float32 [2, 8192, 512], P('group', 'fsdp'), may hold values from -0.018 to 0.018
- adam_second: float32 [2, 8192, 512], P('group', 'fsdp'), may hold values from 1e-06 to 0.0001
- inner_steps: int32 [2], replicated, may hold values from 8 to 128
- group_tokens: int32 [2], replicated, may hold values from 16384 to 131072
- anchor: float32 [8192, 512], P(('fsdp', 'group')), may hold values from -6 to 6
- momentum: float32 [8192, 512], P(('fsdp', 'group')), may hold values from -2 to 2
Outputs:
- new_anchor: float32 [8192, 512], P(('fsdp', 'group'))
- new_momentum: float32 [8192, 512], P(('fsdp', 'group'))
- group_weights: bfloat16 [2, 8192, 512], P('group', 'fsdp')
The draws below stay inside these ranges and needn't reach their ends.
All inputs are finite; a program needn't handle non-finite values.
Results may differ from the reference program's by a relative error of at most 0.0004.
Values may be sent and summed in bfloat16 or wider, within the bound.
A program may use at most 128 MiB of HBM per device.

```python
import math
import jax
import jax.numpy as jnp

D = 8192
KV = 512
TOK_DEV = 512
TOKG = 8192
N_GROUP = 2
N_FSDP = 16


def strengthened(values, rng, source, target, blocks, factor):
    def block_of(position):
        return (jnp.arange(values.shape[position]) // (values.shape[position] // blocks)).reshape((-1,) + (1,) * (values.ndim - 1 - position))

    first = jax.random.permutation(rng, blocks)[block_of(target)]
    far = (block_of(target) + blocks // 2) % blocks
    return jnp.where((block_of(source) == first) | (block_of(source) == far), factor * values, values)


def shard_levels(key, shape, pieces, low, high):
    def one(position, shards_of):
        heights = jax.random.uniform(jax.random.fold_in(jax.random.fold_in(key, 6), position), (shards_of,), jnp.float32, low / len(pieces), high / len(pieces))
        return jnp.repeat(jnp.exp(heights), shape[position] // shards_of).reshape((-1,) + (1,) * (len(shape) - position - 1))

    gain = one(*pieces[0])
    for cut in pieces[1:]:
        gain = gain * one(*cut)
    return gain


def normal_values(key, shape, deviation, bound, shards=(), held_as=jnp.bfloat16):
    values = jax.random.normal(key, shape, jnp.float32) * deviation
    if len(shards) > 0:
        values = shard_levels(key, shape, shards, -0.22, 0.18) * values
    return jnp.clip(values, min=-bound, max=bound).astype(held_as)


def gaussian_with(own_key, extent, deviation, bound, shards, heavy, kind=jnp.bfloat16):
    array = deviation * jax.random.normal(own_key, extent, jnp.float32)
    if shards:
        array = array * shard_levels(own_key, extent, shards, -0.22, 0.18)
    return jnp.clip(strengthened(array, jax.random.fold_in(own_key, 3), *heavy), -bound, bound).astype(kind)


def setup_inputs(seed: int = 0) -> dict:
    seeds = jax.random.split(jax.random.key(seed), 10)
    return {
        "acts": gaussian_with(seeds[0], (N_GROUP, TOKG, D), 1.0, 6.0, ((0, 2), (1, 16)), (1, 2, 16, 2.0)),
        "cotangent": normal_values(seeds[1], (N_GROUP, TOKG, KV), (0.01 * TOKG ** 0.5), 5.40625, ((0, 2), (1, 16))),
        "inner_params": normal_values(seeds[2], (N_GROUP, D, KV), 1.0, 6.0, ((0, 2), (1, 16)), jnp.float32),
        "adam_first": normal_values(seeds[3], (N_GROUP, D, KV), 0.003, 0.018, ((0, 2), (1, 16)), jnp.float32),
        "adam_second": jnp.clip(jnp.exp(math.log(0.0001) - 4.6051702 * jax.random.uniform(seeds[4], (N_GROUP, D, KV), jnp.float32) ** shard_levels(seeds[4], (N_GROUP, D, KV), ((0, 2), (1, 16)), -0.2, 0.2)), 9.999999974752427e-07, 0.0001),
        "inner_steps": jax.random.randint(seeds[5], (N_GROUP,), 8, 129).astype(jnp.int32),
        "group_tokens": jax.random.randint(seeds[6], (N_GROUP,), 16384, 131073).astype(jnp.int32),
        "anchor": normal_values(seeds[7], (D, KV), 1.0, 6.0, ((0, 32),), jnp.float32),
        "momentum": normal_values(seeds[8], (D, KV), 0.3, 2.0, ((0, 32),), jnp.float32),
    }


beta_one = 0.9
beta_two = 0.95
epsilon = 1e-08
inner_rate = 0.3
decay_rate = 0.1
outer_rate = 0.7
outer_mom = 0.9

def inner_update(params, first_moment, second_moment, gradient, steps):
    fresh_first = beta_one * first_moment + (1.0 - beta_one) * gradient
    fresh_second = beta_two * second_moment + (1.0 - beta_two) * gradient * gradient
    steps_float = steps.astype(jnp.float32)
    correct_one = 1.0 - jnp.power(jnp.float32(beta_one), steps_float)
    correct_two = 1.0 - jnp.power(jnp.float32(beta_two), steps_float)
    ratio = fresh_first / correct_one / (jnp.sqrt(fresh_second / correct_two) + epsilon)
    return params - inner_rate * (ratio + decay_rate * params)

def outer_update(anchor, momentum, merged):
    pseudo = anchor - merged
    fresh_momentum = outer_mom * momentum + pseudo
    fresh_anchor = anchor - outer_rate * (pseudo + outer_mom * fresh_momentum)
    return (fresh_anchor, fresh_momentum)

def reference(acts, cotangent, inner_params, adam_first, adam_second, inner_steps, group_tokens, anchor, momentum):
    counts = group_tokens.astype(jnp.float32)
    shares = counts / jnp.sum(counts)
    merged = jnp.zeros((D, KV), jnp.float32)
    for member in range(N_GROUP):
        gradient = jnp.dot(acts[member].T, cotangent[member], preferred_element_type=jnp.float32) / (TOK_DEV * N_FSDP)
        updated = inner_update(inner_params[member], adam_first[member], adam_second[member], gradient, inner_steps[member])
        merged = merged + shares[member] * updated
    new_anchor, new_momentum = outer_update(anchor, momentum, merged)
    group_weights = jnp.broadcast_to(new_anchor.astype(jnp.bfloat16)[None], (N_GROUP, D, KV))
    return (new_anchor, new_momentum, group_weights)
```

```python
import functools

import jax
import jax.numpy as jnp
import numpy as np
from jax import lax
from jax.experimental import pallas as pl
from jax.experimental.pallas import tpu as pltpu
from jax.sharding import PartitionSpec as P

beta_one = 0.9
beta_two = 0.95
epsilon = 1e-08
inner_rate = 0.3
decay_rate = 0.1
outer_rate = 0.7
outer_mom = 0.9


def inner_update(params, first_moment, second_moment, gradient, steps):
    fresh_first = beta_one * first_moment + (1.0 - beta_one) * gradient
    fresh_second = beta_two * second_moment + (1.0 - beta_two) * gradient * gradient
    steps_float = steps.astype(jnp.float32)
    correct_one = 1.0 - jnp.power(jnp.float32(beta_one), steps_float)
    correct_two = 1.0 - jnp.power(jnp.float32(beta_two), steps_float)
    ratio = fresh_first / correct_one / (jnp.sqrt(fresh_second / correct_two) + epsilon)
    return params - inner_rate * (ratio + decay_rate * params)


def outer_update(anchor, momentum, merged):
    pseudo = anchor - merged
    fresh_momentum = outer_mom * momentum + pseudo
    fresh_anchor = anchor - outer_rate * (pseudo + outer_mom * fresh_momentum)
    return (fresh_anchor, fresh_momentum)


def per_device(
    acts,
    cotangent,
    inner_params,
    adam_first,
    adam_second,
    inner_steps,
    group_tokens,
    anchor,
    momentum,
):
    fsdp_count = lax.axis_size("fsdp")
    group_index = lax.axis_index("group")
    inputs = acts[0]
    upstream = cotangent[0]
    group_total = inputs.shape[0] * fsdp_count
    contract = (((0,), (0,)), ((), ()))
    summed = lax.psum_scatter(
        lax.dot_general(inputs, upstream, contract, preferred_element_type=jnp.float32),
        "fsdp",
        scatter_dimension=0,
        tiled=True,
    )
    gradient = summed / group_total
    steps = lax.dynamic_index_in_dim(inner_steps, group_index, 0, False)
    updated = inner_update(inner_params[0], adam_first[0], adam_second[0], gradient, steps)
    counts = group_tokens.astype(jnp.float32)
    share = lax.dynamic_index_in_dim(counts, group_index, 0, False) / jnp.sum(counts)
    weighted = share * updated
    merged = lax.psum_scatter(weighted, "group", scatter_dimension=0, tiled=True)
    new_anchor, new_momentum = outer_update(anchor, momentum, merged)
    rebuilt = lax.all_gather(new_anchor.astype(jnp.bfloat16), "group", axis=0, tiled=True)
    return (new_anchor, new_momentum, rebuilt[None])


MESH = pl.DeviceIdType.MESH
WIRE = jnp.int16
LEVELS = 32767.0
SMALLEST = 1e-30
LINE = 4
FSDP = 16
GROUPS = 2
CORNER_PLAN = (
    ("pass", 1, 0, 0), ("pass", 1, 0, 1), ("cross", 0), ("start_x", 1, 0, 3), ("start_z", 1, 0),
    ("pass", 2, 0, 0), ("pass", 2, 0, 1), ("start_z", 1, 1), ("start_z", 1, 2),
    ("finish", 0, 0), ("finish", 0, 1),
    ("pass", 0, 1, 0), ("pass", 0, 1, 1), ("pass", 1, 1, 0), ("cross", 1), ("start_x", 1, 3, 4),
    ("pass", 1, 1, 1), ("pass", 2, 1, 0), ("pass", 2, 1, 1),
    ("finish", 1, 0), ("finish", 1, 1),
)
MIDDLE_PLAN = (
    ("pass_z", 2, 0), ("pass_z", 1, 0), ("pass", 0, 0, 0), ("pass", 0, 0, 1), ("cross", 0), ("start_x", 1, 0, 3),
    ("pass", 1, 0, 0), ("pass", 2, 0, 0), ("pass", 2, 0, 1), ("pass", 1, 0, 1),
    ("finish", 0, 0), ("pass_z", 0, 1), ("finish", 0, 1),
    ("pass_z", 2, 1), ("pass_z", 1, 1), ("cross", 1), ("start_x", 1, 3, 4),
    ("pass", 0, 1, 0), ("pass", 0, 1, 1), ("pass", 1, 1, 0), ("pass", 2, 1, 0), ("pass", 1, 1, 1), ("pass", 2, 1, 1),
    ("finish", 1, 0), ("finish", 1, 1),
)


def outer_step_kernel(
    group_total,
    steps_in,
    tokens_in,
    acts,
    cotangent,
    params_in,
    first_in,
    second_in,
    anchor_in,
    momentum_in,
    anchor_out,
    momentum_out,
    weights_out,
    steps_smem,
    tokens_smem,
    acts_buf,
    cot_buf,
    cot_t,
    own,
    far_z,
    x_send,
    x_recv,
    x_send_scale,
    x_recv_scale,
    z_send,
    z_send_scale,
    down_recv,
    down_scale,
    up_recv,
    up_scale,
    zz_send,
    zz_send_scale,
    down_z,
    down_z_scale,
    up_z,
    up_z_scale,
    cross_send,
    cross_recv,
    cross_send_scale,
    cross_recv_scale,
    params,
    first,
    second,
    anchor,
    momentum,
    weighted_send,
    weighted_recv,
    fresh_send,
    fresh_recv,
    local_sem,
    acts_send_sem,
    acts_recv_sem,
    cot_sem,
    state_sem,
    x_send_sem,
    x_recv_sem,
    z_send_sem,
    down_sem,
    up_sem,
    zz_send_sem,
    down_z_sem,
    up_z_sem,
    cross_sem,
    weighted_sem,
    fresh_sem,
):
    tokens, _ = acts.shape
    rows, width = params.shape
    half = rows // 2
    wide = width // 2
    line_width = width // 8
    cuts = ((0, wide), (wide, width - line_width))
    tail = slice(width - line_width, width)
    me = lax.axis_index("fsdp")
    group = lax.axis_index("group")
    other_group = 1 - group
    core, x, z = me % 2, (me // 2) % 2, me // 4
    lower = z < 2
    corner = (z == 0) | (z == LINE - 1)
    middle = jnp.logical_not(corner)
    toward = jnp.where(lower, 1, -1)

    sibling = (group, me + 1 - 2 * core)
    across = (group, me + 2 - 4 * x)
    above = (group, me + 4 * toward)
    below = (group, me - 4 * toward)
    peer = (other_group, me)

    def place(n):
        mid = jnp.where(n == 0, 3, jnp.where(n == 1, 0, jnp.where(n == 2, 2, 1)))
        level = jnp.where(corner, 3 - n, mid)
        return jnp.where(lower, level, 3 - level)

    def half_of(i):
        return (other_group + i) % 2

    def columns(n, far, i, owner_core):
        owner_x = jnp.where(far == 1, 1 - x, x)
        block = (place(n) * 2 + owner_x) * 2 + owner_core
        return pl.ds(pl.multiple_of(block * rows + half_of(i) * half, half), half)

    def acts_local(n, i, far):
        return pltpu.make_async_copy(
            acts.at[:, columns(n, far, i, core)],
            acts_buf.at[i, n, far, pl.ds(0, tokens)],
            local_sem.at[i, n, far],
        )

    def acts_remote(n, i, far):
        return pltpu.make_async_remote_copy(
            src_ref=acts.at[:, columns(n, far, i, 1 - core)],
            dst_ref=acts_buf.at[i, n, far, pl.ds(tokens, tokens)],
            send_sem=acts_send_sem.at[i, n, far],
            recv_sem=acts_recv_sem.at[i, n, far],
            device_id=sibling,
            device_id_type=MESH,
        )

    def remote(src, dst, send_sem, recv_sem, target):
        return pltpu.make_async_remote_copy(
            src_ref=src, dst_ref=dst, send_sem=send_sem, recv_sem=recv_sem, device_id=target, device_id_type=MESH
        )

    def x_copies(n, i, p):
        lo, hi = cuts[p]
        return (
            remote(
                x_send_scale.at[n, i, p], x_recv_scale.at[n, i, p],
                x_send_sem.at[n, i, p, 0], x_recv_sem.at[n, i, p, 0], across,
            ),
            remote(
                x_send.at[n, i, pl.ds(lo, hi - lo)], x_recv.at[n, i, pl.ds(lo, hi - lo)],
                x_send_sem.at[n, i, p, 1], x_recv_sem.at[n, i, p, 1], across,
            ),
        )

    def line_copies(n, i, p, into, scale, sem, slot, target):
        lo, hi = cuts[p]
        return (
            remote(
                z_send_scale.at[n, i, p], scale.at[slot, i, p],
                z_send_sem.at[n, i, p, 0], sem.at[slot, i, p, 0], target,
            ),
            remote(
                z_send.at[n, i, pl.ds(lo, hi - lo)], into.at[slot, i, pl.ds(lo, hi - lo)],
                z_send_sem.at[n, i, p, 1], sem.at[slot, i, p, 1], target,
            ),
        )

    def line_z_copies(n, i, into, scale, sem, slot, target):
        return (
            remote(
                zz_send_scale.at[n, i], scale.at[slot, i],
                zz_send_sem.at[n, i, 0], sem.at[slot, i, 0], target,
            ),
            remote(
                zz_send.at[n, i], into.at[slot, i],
                zz_send_sem.at[n, i, 1], sem.at[slot, i, 1], target,
            ),
        )

    def corner_send(n, i, p):
        return line_copies(n, i, p, down_recv, down_scale, down_sem, n, above)

    def middle_send(n, i, p):
        if n == 1:
            return line_copies(n, i, p, up_recv, up_scale, up_sem, 0, below)
        return line_copies(n, i, p, up_recv, up_scale, up_sem, n // 2, above)

    def corner_send_z(n, i):
        return line_z_copies(n, i, down_z, down_z_scale, down_z_sem, n, above)

    def middle_send_z(n, i):
        if n == 1:
            return line_z_copies(n, i, up_z, up_z_scale, up_z_sem, 0, below)
        return line_z_copies(n, i, up_z, up_z_scale, up_z_sem, n // 2, above)

    def from_below(slot, i, p):
        return line_copies(slot, i, p, down_recv, down_scale, down_sem, slot, below)

    def from_above(slot, i, p):
        return line_copies(slot, i, p, up_recv, up_scale, up_sem, slot, above)

    def cross_copies(i):
        return (
            remote(
                cross_send_scale.at[i], cross_recv_scale.at[i],
                cross_sem.at[0, i, 0], cross_sem.at[1, i, 0], across,
            ),
            remote(
                cross_send.at[i], cross_recv.at[i],
                cross_sem.at[0, i, 1], cross_sem.at[1, i, 1], across,
            ),
        )

    def weighted_copy(h):
        return remote(
            weighted_send.at[h], weighted_recv.at[h], weighted_sem.at[0, h], weighted_sem.at[1, h], peer
        )

    def fresh_copy(h):
        return remote(fresh_send.at[h], fresh_recv.at[h], fresh_sem.at[0, h], fresh_sem.at[1, h], peer)

    def start(copies):
        for copy in copies:
            copy.start()

    def arrived(copies):
        for copy in copies:
            copy.wait_recv()

    def left(copies):
        for copy in copies:
            copy.wait_send()

    state = []
    for n, (src, dst) in enumerate(
        (
            (params_in, params), (first_in, first), (second_in, second), (anchor_in, anchor), (momentum_in, momentum),
            (steps_in, steps_smem), (tokens_in, tokens_smem),
        )
    ):
        state.append(pltpu.make_async_copy(src, dst, state_sem.at[n]))
    cot_local = pltpu.make_async_copy(cotangent, cot_buf.at[pl.ds(0, tokens)], cot_sem.at[0])
    cot_remote = pltpu.make_async_remote_copy(
        src_ref=cotangent,
        dst_ref=cot_buf.at[pl.ds(tokens, tokens)],
        send_sem=cot_sem.at[1],
        recv_sem=cot_sem.at[2],
        device_id=sibling,
        device_id_type=MESH,
    )

    barrier = pltpu.get_barrier_semaphore()
    for target in (sibling, across, above, peer):
        pl.semaphore_signal(barrier, inc=1, device_id=target, device_id_type=MESH)

    @pl.when(middle)
    def _():
        pl.semaphore_signal(barrier, inc=1, device_id=below, device_id_type=MESH)

    order = [(n, i, far) for i in range(2) for n in range(LINE) for far in (1, 0)]
    cot_local.start()
    for n, i, far in order:
        acts_local(n, i, far).start()
    for copy in state:
        copy.start()
    pl.semaphore_wait(barrier, jnp.where(middle, 5, 4))
    cot_remote.start()
    for n, i, far in order:
        acts_remote(n, i, far).start()

    def encode(value):
        top = jnp.max(jnp.abs(value), axis=0, keepdims=True)
        levels = jnp.where(top > SMALLEST, LEVELS / jnp.maximum(top, SMALLEST), 0.0)
        return jnp.round(value * levels).astype(jnp.int32).astype(WIRE), top * (1.0 / LEVELS)

    def decode(coded, scale):
        return coded.astype(jnp.int32).astype(jnp.float32) * scale

    cot_local.wait()
    cot_t[:, 0:tokens] = cot_buf[0:tokens].astype(jnp.float32).T.astype(jnp.bfloat16)
    cot_remote.wait_recv()
    cot_t[:, tokens:] = cot_buf[tokens:].astype(jnp.float32).T.astype(jnp.bfloat16)

    def multiply(i):
        @pl.loop(0, LINE)
        def _(n):
            acts_local(n, i, 1).wait()
            acts_remote(n, i, 1).wait_recv()
            product = jnp.dot(cot_t[...], acts_buf[i, n, 1], preferred_element_type=jnp.float32)
            for p, (lo, hi) in enumerate(cuts):
                x_send[n, i, lo:hi], x_send_scale[n, i, p] = encode(product[lo:hi])
                if i == 0:
                    start(x_copies(n, i, p))
            far_z[n, i] = product[tail]
            acts_local(n, i, 0).wait()
            acts_remote(n, i, 0).wait_recv()
            own[n, i] = jnp.dot(cot_t[...], acts_buf[i, n, 0], preferred_element_type=jnp.float32)

            @pl.when(corner & (n < LINE - 1))
            def _():
                zz_send[n, i, 0], zz_send_scale[n, i, 0] = encode(own[n, i, tail])
                zz_send[n, i, 1], zz_send_scale[n, i, 1] = encode(far_z[n, i])
                if i == 0:
                    start(corner_send_z(n, i))

    def received(n, i, p):
        lo, hi = cuts[p]
        arrived(x_copies(n, i, p))
        return own[n, i, lo:hi] + decode(x_recv[n, i, lo:hi], x_recv_scale[n, i, p])

    def plus_line(total, n, i, p, into, scale, sem, slot, source):
        lo, hi = cuts[p]
        arrived(line_copies(0, i, p, into, scale, sem, slot, source))
        return total + decode(into[slot, i, lo:hi], scale[slot, i, p])

    def plus_below(total, i, p, slot):
        return plus_line(total, 0, i, p, down_recv, down_scale, down_sem, slot, below)

    def plus_above(total, i, p, slot):
        return plus_line(total, 0, i, p, up_recv, up_scale, up_sem, slot, above)

    def hand_on(role, n, i, p):
        lo, hi = cuts[p]
        total = received(n, i, p)
        if role == "middle":
            total = plus_above(total, i, p, 0) if n == 1 else plus_below(total, i, p, n // 2)
        z_send[n, i, lo:hi], z_send_scale[n, i, p] = encode(total)
        start(corner_send(n, i, p) if role == "corner" else middle_send(n, i, p))

    def line_z(i, above_slot, below_slot, n):
        if above_slot is not None:
            arrived(line_z_copies(0, i, up_z, up_z_scale, up_z_sem, above_slot, above))
        if below_slot is not None:
            arrived(line_z_copies(0, i, down_z, down_z_scale, down_z_sem, below_slot, below))
        totals = []
        for far in range(2):
            total = far_z[n, i] if far else own[n, i, tail]
            if above_slot is not None:
                total += decode(up_z[above_slot, i, far], up_z_scale[above_slot, i, far])
            if below_slot is not None:
                total += decode(down_z[below_slot, i, far], down_z_scale[below_slot, i, far])
            totals.append(total)
        return totals

    def hand_on_z(n, i):
        totals = line_z(i, 0, None, n) if n == 1 else line_z(i, None, n // 2, n)
        for far in range(2):
            zz_send[n, i, far], zz_send_scale[n, i, far] = encode(totals[far])
        start(middle_send_z(n, i))

    def cross_over(role, i):
        totals = line_z(i, 0, None, 3) if role == "corner" else line_z(i, 1, 2, 3)
        cross_send[i], cross_send_scale[i] = encode(totals[1])
        start(cross_copies(i))
        own[3, i, tail] = totals[0]

    def correction(beta):
        count = jnp.full((1, wide), steps_smem[group], jnp.int32).astype(jnp.float32)
        return 1.0 - jnp.exp(count * float(np.log(np.float64(np.float32(beta)))))

    def share_of(at):
        return jnp.full((1, wide), tokens_smem[at], jnp.int32).astype(jnp.float32)

    def finish(role, i, h):
        total = received(3, i, h)
        if role == "corner":
            total = plus_above(total, i, h, 0)
        else:
            total = plus_above(total, i, h, 1)
            total = plus_below(total, i, h, 2)
        if h == 1:
            arrived(cross_copies(i))
            total = jnp.concatenate([total, own[3, i, tail] + decode(cross_recv[i], cross_recv_scale[i])], axis=0)
        lanes = slice(h * wide, (h + 1) * wide)
        gradient = total.T / group_total
        at = pl.ds(pl.multiple_of(half_of(i) * half, half), half)
        weights = params[at, lanes]
        fresh_first = beta_one * first[at, lanes] + (1.0 - beta_one) * gradient
        fresh_second = beta_two * second[at, lanes] + (1.0 - beta_two) * gradient * gradient
        ratio = fresh_first / correction(beta_one) / (jnp.sqrt(fresh_second / correction(beta_two)) + epsilon)
        share = share_of(group) / (share_of(0) + share_of(1))
        weighted = share * (weights - inner_rate * (ratio + decay_rate * weights))
        if i == 0:
            weighted_send[h] = weighted
            weighted_copy(h).start()
            return
        weighted_copy(h).wait_recv()
        new_anchor, new_momentum = outer_update(anchor[:, lanes], momentum[:, lanes], weighted + weighted_recv[h])
        rounded = new_anchor.astype(jnp.bfloat16)
        fresh_send[h] = rounded
        fresh_copy(h).start()
        anchor_out[:, lanes] = new_anchor
        momentum_out[:, lanes] = new_momentum
        weights_out[at, lanes] = rounded

    def run(role, plan):
        for event in plan:
            kind, rest = event[0], event[1:]
            if kind == "pass":
                hand_on(role, *rest)
            elif kind == "pass_z":
                hand_on_z(*rest)
            elif kind == "cross":
                cross_over(role, *rest)
            elif kind == "start_x":
                for n in range(*rest[1:]):
                    for p in range(2):
                        start(x_copies(n, rest[0], p))
            elif kind == "start_z":
                start(corner_send_z(rest[1], rest[0]))
            else:
                finish(role, *rest)

    multiply(0)

    @pl.when(corner)
    def _():
        run("corner", (("pass", 0, 0, 0), ("pass", 0, 0, 1)))

    @pl.when(middle)
    def _():
        run("middle", (("pass_z", 0, 0),))

    for copy in state:
        copy.wait()
    multiply(1)

    @pl.when(corner)
    def _():
        run("corner", CORNER_PLAN)

    @pl.when(middle)
    def _():
        run("middle", MIDDLE_PLAN)

    theirs = pl.ds(pl.multiple_of(other_group * half, half), half)
    for h in range(2):
        fresh_copy(h).wait_recv()
        weights_out[theirs, h * wide : (h + 1) * wide] = fresh_recv[h]

    cot_remote.wait_send()
    for n, i, far in order:
        acts_remote(n, i, far).wait_send()
    for i in range(2):
        left(cross_copies(i))
        for n in range(LINE):
            for p in range(2):
                left(x_copies(n, i, p))
        for n in range(LINE - 1):
            left(line_z_copies(n, i, down_z, down_z_scale, down_z_sem, n, above))
            for p in range(2):
                left(corner_send(n, i, p))
    for h in range(2):
        weighted_copy(h).wait_send()
        fresh_copy(h).wait_send()


def write_out_kernel(anchor, momentum, weights, anchor_out, momentum_out, weights_out, sem):
    copies = [
        pltpu.make_async_copy(src, dst, sem.at[n])
        for n, (src, dst) in enumerate(((anchor, anchor_out), (momentum, momentum_out), (weights, weights_out)))
    ]
    for copy in copies:
        copy.start()
    for copy in copies:
        copy.wait()


def fused_per_device(
    acts, cotangent, inner_params, adam_first, adam_second, inner_steps, group_tokens, anchor, momentum
):
    tokens, _ = acts.shape[1:]
    rows, width = inner_params.shape[1:]
    half, wide, line_width = rows // 2, width // 2, width // 8
    low, full = jnp.bfloat16, jnp.float32
    dma = pltpu.SemaphoreType.DMA
    vmem = pltpu.VMEM
    body = width - line_width
    results = pl.pallas_call(
        functools.partial(outer_step_kernel, tokens * lax.axis_size("fsdp")),
        out_shape=(
            vmem(anchor.shape, full),
            vmem(anchor.shape, full),
            vmem((rows, width), low),
        ),
        in_specs=[pl.BlockSpec(memory_space=pl.ANY)] * 9,
        out_specs=[pl.BlockSpec(memory_space=pltpu.VMEM)] * 3,
        scratch_shapes=[
            pltpu.SMEM(inner_steps.shape, jnp.int32),
            pltpu.SMEM(group_tokens.shape, jnp.int32),
            vmem((2, LINE, 2, 2 * tokens, half), low),
            vmem((2 * tokens, width), low),
            vmem((width, 2 * tokens), low),
            vmem((LINE, 2, width, half), full),
            vmem((LINE, 2, line_width, half), full),
            vmem((LINE, 2, body, half), WIRE),
            vmem((LINE, 2, body, half), WIRE),
            vmem((LINE, 2, 2, 1, half), full),
            vmem((LINE, 2, 2, 1, half), full),
            vmem((3, 2, body, half), WIRE),
            vmem((3, 2, 2, 1, half), full),
            vmem((3, 2, body, half), WIRE),
            vmem((3, 2, 2, 1, half), full),
            vmem((2, 2, body, half), WIRE),
            vmem((2, 2, 2, 1, half), full),
            vmem((3, 2, 2, line_width, half), WIRE),
            vmem((3, 2, 2, 1, half), full),
            vmem((3, 2, 2, line_width, half), WIRE),
            vmem((3, 2, 2, 1, half), full),
            vmem((2, 2, 2, line_width, half), WIRE),
            vmem((2, 2, 2, 1, half), full),
            vmem((2, line_width, half), WIRE),
            vmem((2, line_width, half), WIRE),
            vmem((2, 1, half), full),
            vmem((2, 1, half), full),
            *[vmem((rows, width), full)] * 3,
            *[vmem((half, width), full)] * 2,
            *[vmem((2, half, wide), full)] * 2,
            *[vmem((2, half, wide), low)] * 2,
            *[dma((2, LINE, 2))] * 3,
            dma((3,)),
            dma((7,)),
            *[dma((LINE, 2, 2, 2))] * 2,
            dma((3, 2, 2, 2)),
            dma((3, 2, 2, 2)),
            dma((2, 2, 2, 2)),
            dma((3, 2, 2)),
            dma((3, 2, 2)),
            dma((2, 2, 2)),
            dma((2, 2, 2)),
            dma((2, 2)),
            dma((2, 2)),
        ],
        compiler_params=pltpu.CompilerParams(
            collective_id=0, has_side_effects=True, vmem_limit_bytes=48 * 1024 * 1024
        ),
    )(
        inner_steps, group_tokens, acts[0], cotangent[0], inner_params[0], adam_first[0], adam_second[0],
        anchor, momentum,
    )
    new_anchor, new_momentum, weights = pl.pallas_call(
        write_out_kernel,
        out_shape=(
            jax.ShapeDtypeStruct(anchor.shape, full),
            jax.ShapeDtypeStruct(anchor.shape, full),
            jax.ShapeDtypeStruct((rows, width), low),
        ),
        in_specs=[pl.BlockSpec(memory_space=pltpu.VMEM)] * 3,
        out_specs=[pl.BlockSpec(memory_space=pl.ANY)] * 3,
        scratch_shapes=[dma((3,))],
        compiler_params=pltpu.CompilerParams(vmem_limit_bytes=4 * 1024 * 1024),
    )(*results)
    return (new_anchor, new_momentum, weights[None])


def choose(*arguments):
    rows, width = arguments[2].shape[1:]
    fits = lax.axis_size("fsdp") == FSDP and lax.axis_size("group") == GROUPS
    if fits and rows % 256 == 0 and width % 256 == 0:
        return fused_per_device(*arguments)
    return per_device(*arguments)


def solution(mesh):
    placed = (
        P("group", "fsdp", None),
        P("group", "fsdp", None),
        P("group", "fsdp", None),
        P("group", "fsdp", None),
        P("group", "fsdp", None),
        P(),
        P(),
        P(("fsdp", "group"), None),
        P(("fsdp", "group"), None),
    )
    return jax.shard_map(
        choose,
        mesh=mesh,
        in_specs=placed,
        out_specs=(
            P(("fsdp", "group"), None),
            P(("fsdp", "group"), None),
            P("group", "fsdp", None),
        ),
        check_vma=False,
    )
```

```python
import functools

import jax
import jax.numpy as jnp
import numpy as np
from jax import lax
from jax.experimental import pallas as pl
from jax.experimental.pallas import tpu as pltpu
from jax.sharding import PartitionSpec as P

beta_one = 0.9
beta_two = 0.95
epsilon = 1e-08
inner_rate = 0.3
decay_rate = 0.1
outer_rate = 0.7
outer_mom = 0.9


def inner_update(params, first_moment, second_moment, gradient, steps):
    fresh_first = beta_one * first_moment + (1.0 - beta_one) * gradient
    fresh_second = beta_two * second_moment + (1.0 - beta_two) * gradient * gradient
    steps_float = steps.astype(jnp.float32)
    correct_one = 1.0 - jnp.power(jnp.float32(beta_one), steps_float)
    correct_two = 1.0 - jnp.power(jnp.float32(beta_two), steps_float)
    ratio = fresh_first / correct_one / (jnp.sqrt(fresh_second / correct_two) + epsilon)
    return params - inner_rate * (ratio + decay_rate * params)


def outer_update(anchor, momentum, merged):
    pseudo = anchor - merged
    fresh_momentum = outer_mom * momentum + pseudo
    fresh_anchor = anchor - outer_rate * (pseudo + outer_mom * fresh_momentum)
    return (fresh_anchor, fresh_momentum)


def per_device(
    acts,
    cotangent,
    inner_params,
    adam_first,
    adam_second,
    inner_steps,
    group_tokens,
    anchor,
    momentum,
):
    fsdp_count = lax.axis_size("fsdp")
    group_index = lax.axis_index("group")
    inputs = acts[0]
    upstream = cotangent[0]
    group_total = inputs.shape[0] * fsdp_count
    contract = (((0,), (0,)), ((), ()))
    summed = lax.psum_scatter(
        lax.dot_general(inputs, upstream, contract, preferred_element_type=jnp.float32),
        "fsdp",
        scatter_dimension=0,
        tiled=True,
    )
    gradient = summed / group_total
    steps = lax.dynamic_index_in_dim(inner_steps, group_index, 0, False)
    updated = inner_update(inner_params[0], adam_first[0], adam_second[0], gradient, steps)
    counts = group_tokens.astype(jnp.float32)
    share = lax.dynamic_index_in_dim(counts, group_index, 0, False) / jnp.sum(counts)
    weighted = share * updated
    merged = lax.psum_scatter(weighted, "group", scatter_dimension=0, tiled=True)
    new_anchor, new_momentum = outer_update(anchor, momentum, merged)
    rebuilt = lax.all_gather(new_anchor.astype(jnp.bfloat16), "group", axis=0, tiled=True)
    return (new_anchor, new_momentum, rebuilt[None])


MESH = pl.DeviceIdType.MESH
WIRE = jnp.int16
LEVELS = 32767.0
SMALLEST = 1e-30
LINE = 4
LINE_SHARE = 3
FSDP = 16
GROUPS = 2
CORNER_PLAN = (
    ("pass", 1, 0, 0), ("pass", 1, 0, 1), ("cross", 0), ("start_x", 1, 0, 3),
    ("pass", 2, 0, 0), ("pass", 2, 0, 1), ("finish", 0, 0), ("finish", 0, 1),
    ("pass", 0, 1, 0), ("pass", 0, 1, 1), ("cross", 1), ("start_x", 1, 3, 4),
    ("pass", 1, 1, 0), ("pass", 1, 1, 1), ("pass", 2, 1, 0), ("pass", 2, 1, 1),
    ("finish", 1, 0), ("finish", 1, 1),
)
MIDDLE_PLAN = (
    ("pass_z", 2, 0), ("pass_z", 1, 0), ("pass", 0, 0, 0), ("pass", 0, 0, 1), ("pass_z", 0, 1),
    ("cross", 0), ("start_x", 1, 0, 3), ("pass_z", 2, 1), ("pass", 1, 0, 0), ("pass", 2, 0, 0),
    ("pass", 1, 0, 1), ("pass_z", 1, 1), ("pass", 2, 0, 1), ("cross", 1), ("start_x", 1, 3, 4),
    ("finish", 0, 0), ("finish", 0, 1),
    ("pass", 0, 1, 0), ("pass", 0, 1, 1), ("pass", 2, 1, 0), ("pass", 1, 1, 0), ("pass", 1, 1, 1), ("pass", 2, 1, 1),
    ("finish", 1, 0), ("finish", 1, 1),
)


def line_width_of(width):
    return width * LINE_SHARE // 256 * 16


def outer_step_kernel(
    group_total,
    steps_in,
    tokens_in,
    acts,
    cotangent,
    params_in,
    first_in,
    second_in,
    anchor_in,
    momentum_in,
    anchor_out,
    momentum_out,
    weights_out,
    steps_smem,
    tokens_smem,
    acts_buf,
    cot_buf,
    cot_t,
    own,
    far_z,
    x_send,
    x_recv,
    x_send_scale,
    x_recv_scale,
    z_send,
    z_send_scale,
    down_recv,
    down_scale,
    up_recv,
    up_scale,
    zz_send,
    zz_send_scale,
    down_z,
    down_z_scale,
    up_z,
    up_z_scale,
    cross_send,
    cross_recv,
    cross_send_scale,
    cross_recv_scale,
    params,
    first,
    second,
    anchor,
    momentum,
    weighted_send,
    weighted_recv,
    fresh_send,
    fresh_recv,
    local_sem,
    acts_send_sem,
    acts_recv_sem,
    cot_sem,
    state_sem,
    x_send_sem,
    x_recv_sem,
    z_send_sem,
    down_sem,
    up_sem,
    zz_send_sem,
    down_z_sem,
    up_z_sem,
    cross_send_sem,
    cross_recv_sem,
    weighted_sem,
    fresh_sem,
):
    tokens, _ = acts.shape
    rows, width = params.shape
    half = rows // 2
    wide = width // 2
    line_width = line_width_of(width)
    cuts = ((0, wide), (wide, width - line_width))
    tail = slice(width - line_width, width)
    me = lax.axis_index("fsdp")
    group = lax.axis_index("group")
    other_group = 1 - group
    core, x, z = me % 2, (me // 2) % 2, me // 4
    lower = z < 2
    corner = (z == 0) | (z == LINE - 1)
    middle = jnp.logical_not(corner)
    toward = jnp.where(lower, 1, -1)

    sibling = (group, me + 1 - 2 * core)
    across = (group, me + 2 - 4 * x)
    above = (group, me + 4 * toward)
    below = (group, me - 4 * toward)
    peer = (other_group, me)

    def place(n):
        mid = jnp.where(n == 0, 3, jnp.where(n == 1, 0, jnp.where(n == 2, 2, 1)))
        level = jnp.where(corner, 3 - n, mid)
        return jnp.where(lower, level, 3 - level)

    def half_of(i):
        return (other_group + i) % 2

    def columns(n, far, i, owner_core):
        owner_x = jnp.where(far == 1, 1 - x, x)
        block = (place(n) * 2 + owner_x) * 2 + owner_core
        return pl.ds(pl.multiple_of(block * rows + half_of(i) * half, half), half)

    def acts_local(n, i, far):
        return pltpu.make_async_copy(
            acts.at[:, columns(n, far, i, core)],
            acts_buf.at[i, n, far, pl.ds(0, tokens)],
            local_sem.at[i, n, far],
        )

    def acts_remote(n, i, far):
        return pltpu.make_async_remote_copy(
            src_ref=acts.at[:, columns(n, far, i, 1 - core)],
            dst_ref=acts_buf.at[i, n, far, pl.ds(tokens, tokens)],
            send_sem=acts_send_sem,
            recv_sem=acts_recv_sem.at[i, n, far],
            device_id=sibling,
            device_id_type=MESH,
        )

    def remote(src, dst, send_sem, recv_sem, target):
        return pltpu.make_async_remote_copy(
            src_ref=src, dst_ref=dst, send_sem=send_sem, recv_sem=recv_sem, device_id=target, device_id_type=MESH
        )

    def x_copies(n, i, p):
        lo, hi = cuts[p]
        return (
            remote(
                x_send_scale.at[n, i, p], x_recv_scale.at[n, i, p],
                x_send_sem.at[0], x_recv_sem.at[n, i, p, 0], across,
            ),
            remote(
                x_send.at[n, i, pl.ds(lo, hi - lo)], x_recv.at[n, i, pl.ds(lo, hi - lo)],
                x_send_sem.at[1], x_recv_sem.at[n, i, p, 1], across,
            ),
        )

    def line_copies(n, i, p, into, scale, sem, slot, target):
        lo, hi = cuts[p]
        return (
            remote(
                z_send_scale.at[n, i, p], scale.at[slot, i, p],
                z_send_sem.at[0], sem.at[slot, i, p, 0], target,
            ),
            remote(
                z_send.at[n, i, pl.ds(lo, hi - lo)], into.at[slot, i, pl.ds(lo, hi - lo)],
                z_send_sem.at[1], sem.at[slot, i, p, 1], target,
            ),
        )

    def line_z_copies(n, i, into, scale, sem, slot, target):
        return (
            remote(
                zz_send_scale.at[n, i], scale.at[slot, i],
                zz_send_sem.at[0], sem.at[slot, i, 0], target,
            ),
            remote(
                zz_send.at[n, i], into.at[slot, i],
                zz_send_sem.at[1], sem.at[slot, i, 1], target,
            ),
        )

    def corner_send(n, i, p):
        return line_copies(n, i, p, down_recv, down_scale, down_sem, n, above)

    def middle_send(n, i, p):
        if n == 1:
            return line_copies(n, i, p, up_recv, up_scale, up_sem, 0, below)
        return line_copies(n, i, p, up_recv, up_scale, up_sem, n // 2, above)

    def corner_send_z(n, i):
        return line_z_copies(n, i, down_z, down_z_scale, down_z_sem, n, above)

    def middle_send_z(n, i):
        if n == 1:
            return line_z_copies(n, i, up_z, up_z_scale, up_z_sem, 0, below)
        return line_z_copies(n, i, up_z, up_z_scale, up_z_sem, n // 2, above)

    def from_below(slot, i, p):
        return line_copies(slot, i, p, down_recv, down_scale, down_sem, slot, below)

    def from_above(slot, i, p):
        return line_copies(slot, i, p, up_recv, up_scale, up_sem, slot, above)

    def cross_copies(i):
        return (
            remote(
                cross_send_scale.at[i], cross_recv_scale.at[i],
                cross_send_sem.at[0], cross_recv_sem.at[i, 0], across,
            ),
            remote(
                cross_send.at[i], cross_recv.at[i],
                cross_send_sem.at[1], cross_recv_sem.at[i, 1], across,
            ),
        )

    def weighted_copy(h):
        return remote(
            weighted_send.at[h], weighted_recv.at[h], weighted_sem.at[2], weighted_sem.at[h], peer
        )

    def fresh_copy(h):
        return remote(fresh_send.at[h], fresh_recv.at[h], fresh_sem.at[2], fresh_sem.at[h], peer)

    def start(copies):
        for copy in copies:
            copy.start()

    def arrived(copies):
        for copy in copies:
            copy.wait_recv()

    state = []
    for n, (src, dst) in enumerate(
        (
            (params_in, params), (first_in, first), (second_in, second), (anchor_in, anchor), (momentum_in, momentum),
            (steps_in, steps_smem), (tokens_in, tokens_smem),
        )
    ):
        state.append(pltpu.make_async_copy(src, dst, state_sem.at[n]))
    cot_local = pltpu.make_async_copy(cotangent, cot_buf.at[pl.ds(0, tokens)], cot_sem.at[0])
    cot_remote = pltpu.make_async_remote_copy(
        src_ref=cotangent,
        dst_ref=cot_buf.at[pl.ds(tokens, tokens)],
        send_sem=cot_sem.at[1],
        recv_sem=cot_sem.at[2],
        device_id=sibling,
        device_id_type=MESH,
    )

    barrier = pltpu.get_barrier_semaphore()
    for target in (sibling, across, above, peer):
        pl.semaphore_signal(barrier, inc=1, device_id=target, device_id_type=MESH)

    @pl.when(middle)
    def _():
        pl.semaphore_signal(barrier, inc=1, device_id=below, device_id_type=MESH)

    order = [(n, i, far) for i in range(2) for n in range(LINE) for far in (1, 0)]
    cot_local.start()
    for n, i, far in order:
        acts_local(n, i, far).start()
    for copy in state:
        copy.start()
    pl.semaphore_wait(barrier, jnp.where(middle, 5, 4))
    cot_remote.start()
    for n, i, far in order:
        acts_remote(n, i, far).start()

    def encode(value):
        top = jnp.max(jnp.abs(value), axis=0, keepdims=True)
        levels = jnp.where(top > SMALLEST, LEVELS / jnp.maximum(top, SMALLEST), 0.0)
        return jnp.round(value * levels).astype(jnp.int32).astype(WIRE), top * (1.0 / LEVELS)

    def decode(coded, scale):
        return coded.astype(jnp.int32).astype(jnp.float32) * scale

    cot_local.wait()
    cot_t[:, 0:tokens] = cot_buf[0:tokens].astype(jnp.float32).T.astype(jnp.bfloat16)
    cot_remote.wait_recv()
    cot_t[:, tokens:] = cot_buf[tokens:].astype(jnp.float32).T.astype(jnp.bfloat16)

    def multiply(i):
        @pl.loop(0, LINE)
        def _(n):
            acts_local(n, i, 1).wait()
            acts_remote(n, i, 1).wait_recv()
            product = jnp.dot(cot_t[...], acts_buf[i, n, 1], preferred_element_type=jnp.float32)
            for p, (lo, hi) in enumerate(cuts):
                x_send[n, i, lo:hi], x_send_scale[n, i, p] = encode(product[lo:hi])
                if i == 0:
                    start(x_copies(n, i, p))
            far_z[n, i] = product[tail]
            acts_local(n, i, 0).wait()
            acts_remote(n, i, 0).wait_recv()
            own[n, i] = jnp.dot(cot_t[...], acts_buf[i, n, 0], preferred_element_type=jnp.float32)

            @pl.when(corner & (n < LINE - 1))
            def _():
                zz_send[n, i, 0], zz_send_scale[n, i, 0] = encode(own[n, i, tail])
                zz_send[n, i, 1], zz_send_scale[n, i, 1] = encode(far_z[n, i])
                start(corner_send_z(n, i))

    def received(n, i, p):
        lo, hi = cuts[p]
        arrived(x_copies(n, i, p))
        return own[n, i, lo:hi] + decode(x_recv[n, i, lo:hi], x_recv_scale[n, i, p])

    def plus_line(total, n, i, p, into, scale, sem, slot, source):
        lo, hi = cuts[p]
        arrived(line_copies(0, i, p, into, scale, sem, slot, source))
        return total + decode(into[slot, i, lo:hi], scale[slot, i, p])

    def plus_below(total, i, p, slot):
        return plus_line(total, 0, i, p, down_recv, down_scale, down_sem, slot, below)

    def plus_above(total, i, p, slot):
        return plus_line(total, 0, i, p, up_recv, up_scale, up_sem, slot, above)

    def hand_on(role, n, i, p):
        lo, hi = cuts[p]
        total = received(n, i, p)
        if role == "middle":
            total = plus_above(total, i, p, 0) if n == 1 else plus_below(total, i, p, n // 2)
        z_send[n, i, lo:hi], z_send_scale[n, i, p] = encode(total)
        start(corner_send(n, i, p) if role == "corner" else middle_send(n, i, p))

    def line_z(i, above_slot, below_slot, n):
        if above_slot is not None:
            arrived(line_z_copies(0, i, up_z, up_z_scale, up_z_sem, above_slot, above))
        if below_slot is not None:
            arrived(line_z_copies(0, i, down_z, down_z_scale, down_z_sem, below_slot, below))
        totals = []
        for far in range(2):
            total = far_z[n, i] if far else own[n, i, tail]
            if above_slot is not None:
                total += decode(up_z[above_slot, i, far], up_z_scale[above_slot, i, far])
            if below_slot is not None:
                total += decode(down_z[below_slot, i, far], down_z_scale[below_slot, i, far])
            totals.append(total)
        return totals

    def hand_on_z(n, i):
        totals = line_z(i, 0, None, n) if n == 1 else line_z(i, None, n // 2, n)
        for far in range(2):
            zz_send[n, i, far], zz_send_scale[n, i, far] = encode(totals[far])
        start(middle_send_z(n, i))

    def cross_over(role, i):
        totals = line_z(i, 0, None, 3) if role == "corner" else line_z(i, 1, 2, 3)
        cross_send[i], cross_send_scale[i] = encode(totals[1])
        start(cross_copies(i))
        own[3, i, tail] = totals[0]

    def correction(beta):
        count = jnp.full((1, wide), steps_smem[group], jnp.int32).astype(jnp.float32)
        return 1.0 - jnp.exp(count * float(np.log(np.float64(np.float32(beta)))))

    def share_of(at):
        return jnp.full((1, wide), tokens_smem[at], jnp.int32).astype(jnp.float32)

    def finish(role, i, h):
        total = received(3, i, h)
        if role == "corner":
            total = plus_above(total, i, h, 0)
        else:
            total = plus_above(total, i, h, 1)
            total = plus_below(total, i, h, 2)
        if h == 1:
            arrived(cross_copies(i))
            total = jnp.concatenate([total, own[3, i, tail] + decode(cross_recv[i], cross_recv_scale[i])], axis=0)
        lanes = slice(h * wide, (h + 1) * wide)
        gradient = total.T / group_total
        at = pl.ds(pl.multiple_of(half_of(i) * half, half), half)
        weights = params[at, lanes]
        fresh_first = beta_one * first[at, lanes] + (1.0 - beta_one) * gradient
        fresh_second = beta_two * second[at, lanes] + (1.0 - beta_two) * gradient * gradient
        ratio = fresh_first / correction(beta_one) / (jnp.sqrt(fresh_second / correction(beta_two)) + epsilon)
        share = share_of(group) / (share_of(0) + share_of(1))
        weighted = share * (weights - inner_rate * (ratio + decay_rate * weights))
        if i == 0:
            weighted_send[h] = weighted
            weighted_copy(h).start()
            return
        weighted_copy(h).wait_recv()
        new_anchor, new_momentum = outer_update(anchor[:, lanes], momentum[:, lanes], weighted + weighted_recv[h])
        rounded = new_anchor.astype(jnp.bfloat16)
        fresh_send[h] = rounded
        fresh_copy(h).start()
        anchor_out[:, lanes] = new_anchor
        momentum_out[:, lanes] = new_momentum
        weights_out[at, lanes] = rounded

    def run(role, plan):
        for event in plan:
            kind, rest = event[0], event[1:]
            if kind == "pass":
                hand_on(role, *rest)
            elif kind == "pass_z":
                hand_on_z(*rest)
            elif kind == "cross":
                cross_over(role, *rest)
            elif kind == "start_x":
                for n in range(*rest[1:]):
                    for p in range(2):
                        start(x_copies(n, rest[0], p))
            else:
                finish(role, *rest)

    multiply(0)

    @pl.when(corner)
    def _():
        run("corner", (("pass", 0, 0, 0), ("pass", 0, 0, 1)))

    @pl.when(middle)
    def _():
        run("middle", (("pass_z", 0, 0),))

    for copy in state:
        copy.wait()
    multiply(1)

    @pl.when(corner)
    def _():
        run("corner", CORNER_PLAN)

    @pl.when(middle)
    def _():
        run("middle", MIDDLE_PLAN)

    theirs = pl.ds(pl.multiple_of(other_group * half, half), half)
    for h in range(2):
        fresh_copy(h).wait_recv()
        weights_out[theirs, h * wide : (h + 1) * wide] = fresh_recv[h]

    cot_remote.wait_send()
    remote(acts_buf.at[0], acts_buf.at[0], acts_send_sem, acts_send_sem, sibling).wait_send()
    for buffer, sem in (
        (x_send_scale, x_send_sem.at[0]),
        (x_send, x_send_sem.at[1]),
        (z_send_scale, z_send_sem.at[0]),
        (z_send, z_send_sem.at[1]),
        (zz_send_scale, zz_send_sem.at[0]),
        (zz_send, zz_send_sem.at[1]),
        (cross_send_scale, cross_send_sem.at[0]),
        (cross_send, cross_send_sem.at[1]),
        (weighted_send, weighted_sem.at[2]),
        (fresh_send, fresh_sem.at[2]),
    ):
        remote(buffer, buffer, sem, sem, sibling).wait_send()


def write_out_kernel(anchor, momentum, weights, anchor_out, momentum_out, weights_out, sem):
    copies = [
        pltpu.make_async_copy(src, dst, sem.at[n])
        for n, (src, dst) in enumerate(((anchor, anchor_out), (momentum, momentum_out), (weights, weights_out)))
    ]
    for copy in copies:
        copy.start()
    for copy in copies:
        copy.wait()


def fused_per_device(
    acts, cotangent, inner_params, adam_first, adam_second, inner_steps, group_tokens, anchor, momentum
):
    tokens, _ = acts.shape[1:]
    rows, width = inner_params.shape[1:]
    half, wide, line_width = rows // 2, width // 2, line_width_of(width)
    low, full = jnp.bfloat16, jnp.float32
    dma = pltpu.SemaphoreType.DMA
    vmem = pltpu.VMEM
    body = width - line_width
    operands = (
        inner_steps, group_tokens, acts[0], cotangent[0], inner_params[0], adam_first[0], adam_second[0],
        anchor, momentum,
    )
    results = pl.pallas_call(
        functools.partial(outer_step_kernel, tokens * lax.axis_size("fsdp")),
        out_shape=(
            vmem(anchor.shape, full),
            vmem(anchor.shape, full),
            vmem((rows, width), low),
        ),
        in_specs=[pl.BlockSpec(memory_space=pltpu.HBM)] * 9,
        out_specs=[pl.BlockSpec(memory_space=pltpu.VMEM)] * 3,
        scratch_shapes=[
            pltpu.SMEM(inner_steps.shape, jnp.int32),
            pltpu.SMEM(group_tokens.shape, jnp.int32),
            vmem((2, LINE, 2, 2 * tokens, half), low),
            vmem((2 * tokens, width), low),
            vmem((width, 2 * tokens), low),
            vmem((LINE, 2, width, half), full),
            vmem((LINE, 2, line_width, half), full),
            vmem((LINE, 2, body, half), WIRE),
            vmem((LINE, 2, body, half), WIRE),
            vmem((LINE, 2, 2, 1, half), full),
            vmem((LINE, 2, 2, 1, half), full),
            vmem((3, 2, body, half), WIRE),
            vmem((3, 2, 2, 1, half), full),
            vmem((3, 2, body, half), WIRE),
            vmem((3, 2, 2, 1, half), full),
            vmem((2, 2, body, half), WIRE),
            vmem((2, 2, 2, 1, half), full),
            vmem((3, 2, 2, line_width, half), WIRE),
            vmem((3, 2, 2, 1, half), full),
            vmem((3, 2, 2, line_width, half), WIRE),
            vmem((3, 2, 2, 1, half), full),
            vmem((2, 2, 2, line_width, half), WIRE),
            vmem((2, 2, 2, 1, half), full),
            vmem((2, line_width, half), WIRE),
            vmem((2, line_width, half), WIRE),
            vmem((2, 1, half), full),
            vmem((2, 1, half), full),
            *[vmem((rows, width), full)] * 3,
            *[vmem((half, width), full)] * 2,
            *[vmem((2, half, wide), full)] * 2,
            *[vmem((2, half, wide), low)] * 2,
            dma((2, LINE, 2)),
            dma,
            dma((2, LINE, 2)),
            dma((3,)),
            dma((7,)),
            dma((2,)),
            dma((LINE, 2, 2, 2)),
            dma((2,)),
            dma((3, 2, 2, 2)),
            dma((2, 2, 2, 2)),
            dma((2,)),
            dma((3, 2, 2)),
            dma((2, 2, 2)),
            dma((2,)),
            dma((2, 2)),
            dma((3,)),
            dma((3,)),
        ],
        compiler_params=pltpu.CompilerParams(
            collective_id=0, has_side_effects=True, vmem_limit_bytes=48 * 1024 * 1024
        ),
    )(*(pltpu.with_memory_space_constraint(operand, pltpu.HBM) for operand in operands))
    new_anchor, new_momentum, weights = pl.pallas_call(
        write_out_kernel,
        out_shape=(
            jax.ShapeDtypeStruct(anchor.shape, full),
            jax.ShapeDtypeStruct(anchor.shape, full),
            jax.ShapeDtypeStruct((rows, width), low),
        ),
        in_specs=[pl.BlockSpec(memory_space=pltpu.VMEM)] * 3,
        out_specs=[pl.BlockSpec(memory_space=pl.ANY)] * 3,
        scratch_shapes=[dma((3,))],
        compiler_params=pltpu.CompilerParams(vmem_limit_bytes=4 * 1024 * 1024),
    )(*results)
    return (new_anchor, new_momentum, weights[None])


def choose(*arguments):
    rows, width = arguments[2].shape[1:]
    fits = lax.axis_size("fsdp") == FSDP and lax.axis_size("group") == GROUPS
    if fits and rows % 256 == 0 and width % 256 == 0:
        return fused_per_device(*arguments)
    return per_device(*arguments)


def solution(mesh):
    placed = (
        P("group", "fsdp", None),
        P("group", "fsdp", None),
        P("group", "fsdp", None),
        P("group", "fsdp", None),
        P("group", "fsdp", None),
        P(),
        P(),
        P(("fsdp", "group"), None),
        P(("fsdp", "group"), None),
    )
    return jax.shard_map(
        choose,
        mesh=mesh,
        in_specs=placed,
        out_specs=(
            P(("fsdp", "group"), None),
            P(("fsdp", "group"), None),
            P("group", "fsdp", None),
        ),
        check_vma=False,
    )
```

```python
import functools

import jax
import jax.numpy as jnp
import numpy as np
from jax import lax
from jax.experimental import pallas as pl
from jax.experimental.pallas import tpu as pltpu
from jax.sharding import PartitionSpec as P

beta_one = 0.9
beta_two = 0.95
epsilon = 1e-08
inner_rate = 0.3
decay_rate = 0.1
outer_rate = 0.7
outer_mom = 0.9


def inner_update(params, first_moment, second_moment, gradient, steps):
    fresh_first = beta_one * first_moment + (1.0 - beta_one) * gradient
    fresh_second = beta_two * second_moment + (1.0 - beta_two) * gradient * gradient
    steps_float = steps.astype(jnp.float32)
    correct_one = 1.0 - jnp.power(jnp.float32(beta_one), steps_float)
    correct_two = 1.0 - jnp.power(jnp.float32(beta_two), steps_float)
    ratio = fresh_first / correct_one / (jnp.sqrt(fresh_second / correct_two) + epsilon)
    return params - inner_rate * (ratio + decay_rate * params)


def outer_update(anchor, momentum, merged):
    pseudo = anchor - merged
    fresh_momentum = outer_mom * momentum + pseudo
    fresh_anchor = anchor - outer_rate * (pseudo + outer_mom * fresh_momentum)
    return (fresh_anchor, fresh_momentum)


def per_device(
    acts,
    cotangent,
    inner_params,
    adam_first,
    adam_second,
    inner_steps,
    group_tokens,
    anchor,
    momentum,
):
    fsdp_count = lax.axis_size("fsdp")
    group_index = lax.axis_index("group")
    inputs = acts[0]
    upstream = cotangent[0]
    group_total = inputs.shape[0] * fsdp_count
    contract = (((0,), (0,)), ((), ()))
    summed = lax.psum_scatter(
        lax.dot_general(inputs, upstream, contract, preferred_element_type=jnp.float32),
        "fsdp",
        scatter_dimension=0,
        tiled=True,
    )
    gradient = summed / group_total
    steps = lax.dynamic_index_in_dim(inner_steps, group_index, 0, False)
    updated = inner_update(inner_params[0], adam_first[0], adam_second[0], gradient, steps)
    counts = group_tokens.astype(jnp.float32)
    share = lax.dynamic_index_in_dim(counts, group_index, 0, False) / jnp.sum(counts)
    weighted = share * updated
    merged = lax.psum_scatter(weighted, "group", scatter_dimension=0, tiled=True)
    new_anchor, new_momentum = outer_update(anchor, momentum, merged)
    rebuilt = lax.all_gather(new_anchor.astype(jnp.bfloat16), "group", axis=0, tiled=True)
    return (new_anchor, new_momentum, rebuilt[None])


MESH = pl.DeviceIdType.MESH
WIRE = jnp.int16
LEVELS = 32767.0
SMALLEST = 1e-30
LINE = 4
FSDP = 16
GROUPS = 2
MIDDLE_ROUTE = ((1, 0), (0, 1), (1, 2))
CORNER_PLAN = (
    ("pass", 1, 0), ("cross", 0), ("start_x", 1, 0, 3), ("pass", 2, 0),
    ("cross", 1), ("start_x", 1, 3, 4), ("pass", 0, 1), ("finish", 0), ("pass", 1, 1), ("pass", 2, 1), ("finish", 1),
)
MIDDLE_PLAN = (
    ("pass_z", 2, 0), ("pass", 0, 0), ("pass", 1, 0), ("cross", 0), ("start_x", 1, 0, 3), ("pass_z", 0, 1),
    ("pass_z", 2, 1), ("pass", 2, 0), ("cross", 1), ("start_x", 1, 3, 4), ("finish", 0),
    ("pass", 1, 1), ("pass", 0, 1), ("pass", 2, 1), ("finish", 1),
)


def line_width_of(width):
    return width // 16 * 6 // 32 * 16


def cuts_of(width):
    step, last = width // 4, width - line_width_of(width)
    cuts = [(lo, min(lo + step, last)) for lo in range(0, last, step)]
    return (cuts[-1], *cuts[:-1])


def outer_step_kernel(
    group_total,
    steps_in,
    tokens_in,
    acts,
    cotangent,
    params_in,
    first_in,
    second_in,
    anchor_in,
    momentum_in,
    anchor_out,
    momentum_out,
    weights_out,
    steps_smem,
    tokens_smem,
    acts_buf,
    cot_buf,
    cot_t,
    own,
    far_z,
    x_send,
    x_recv,
    x_send_scale,
    x_recv_scale,
    z_send,
    z_send_scale,
    down_recv,
    down_scale,
    up_recv,
    up_scale,
    zz_send,
    zz_send_scale,
    down_z,
    down_z_scale,
    up_z,
    up_z_scale,
    cross_send,
    cross_recv,
    cross_send_scale,
    cross_recv_scale,
    params,
    first,
    second,
    anchor,
    momentum,
    weighted_send,
    weighted_recv,
    fresh_send,
    fresh_recv,
    measure_buf,
    vouch_sem,
    acts_send_sem,
    acts_recv_sem,
    cot_sem,
    state_sem,
    x_send_sem,
    x_recv_sem,
    z_send_sem,
    down_sem,
    up_sem,
    zz_send_sem,
    down_z_sem,
    up_z_sem,
    cross_send_sem,
    cross_recv_sem,
    weighted_sem,
    fresh_sem,
):
    tokens, _ = acts.shape
    rows, width = params.shape
    half = rows // 2
    line_width = line_width_of(width)
    cuts = cuts_of(width)
    parts = len(cuts)
    tail = slice(width - line_width, width)
    me = lax.axis_index("fsdp")
    group = lax.axis_index("group")
    other_group = 1 - group
    core, x, z = me % 2, (me // 2) % 2, me // 4
    lower = z < 2
    corner = (z == 0) | (z == LINE - 1)
    middle = jnp.logical_not(corner)
    toward = jnp.where(lower, 1, -1)

    sibling = (group, me + 1 - 2 * core)
    across = (group, me + 2 - 4 * x)
    above = (group, me + 4 * toward)
    below = (group, me - 4 * toward)
    beyond = (group, me + 8 * toward)
    peer = (other_group, me)

    def place(n):
        mid = jnp.where(n == 0, 3, jnp.where(n == 1, 0, jnp.where(n == 2, 2, 1)))
        level = jnp.where(corner, 3 - n, mid)
        return jnp.where(lower, level, 3 - level)

    def half_of(i):
        return (other_group + i) % 2

    def columns(n, far, i, owner_core):
        owner_x = jnp.where(far == 1, 1 - x, x)
        block = (place(n) * 2 + owner_x) * 2 + owner_core
        return pl.ds(pl.multiple_of(block * rows + half_of(i) * half, half), half)

    def acts_local(n, i, far):
        return pltpu.make_async_copy(
            acts.at[:, columns(n, far, i, core)],
            acts_buf.at[i, n, far, pl.ds(0, tokens)],
            acts_recv_sem.at[i, n, far],
        )

    def acts_remote(n, i, far):
        return pltpu.make_async_remote_copy(
            src_ref=acts.at[:, columns(n, far, i, 1 - core)],
            dst_ref=acts_buf.at[i, n, far, pl.ds(tokens, tokens)],
            send_sem=acts_send_sem,
            recv_sem=acts_recv_sem.at[i, n, far],
            device_id=sibling,
            device_id_type=MESH,
        )

    def acts_arrived(n, i, far):
        whole = acts_buf.at[i, n, far]
        pltpu.make_async_copy(whole, whole, acts_recv_sem.at[i, n, far]).wait()

    def fetch(n, i):
        for far in (1, 0):
            acts_local(n, i, far).start()
            acts_remote(n, i, far).start()

    def remote(src, dst, send_sem, recv_sem, target):
        return pltpu.make_async_remote_copy(
            src_ref=src, dst_ref=dst, send_sem=send_sem, recv_sem=recv_sem, device_id=target, device_id_type=MESH
        )

    def x_copies(n, i, p):
        lo, hi = cuts[p]
        return (
            remote(
                x_send_scale.at[n, i, p], x_recv_scale.at[n, i, p],
                x_send_sem.at[0], x_recv_sem.at[n, i, p], across,
            ),
            remote(
                x_send.at[n, i, pl.ds(lo, hi - lo)], x_recv.at[n, i, pl.ds(lo, hi - lo)],
                x_send_sem.at[1], x_recv_sem.at[n, i, p], across,
            ),
        )

    def line_copies(n, i, p, into, scale, sem, slot, target):
        lo, hi = cuts[p]
        return (
            remote(
                z_send_scale.at[n, i, p], scale.at[slot, i, p],
                z_send_sem.at[0], sem.at[slot, i, p], target,
            ),
            remote(
                z_send.at[n, i, pl.ds(lo, hi - lo)], into.at[slot, i, pl.ds(lo, hi - lo)],
                z_send_sem.at[1], sem.at[slot, i, p], target,
            ),
        )

    def line_z_copies(n, i, into, scale, sem, slot, target):
        return (
            remote(
                zz_send_scale.at[n, i], scale.at[slot, i],
                zz_send_sem.at[0], sem.at[slot, i], target,
            ),
            remote(
                zz_send.at[n, i], into.at[slot, i],
                zz_send_sem.at[1], sem.at[slot, i], target,
            ),
        )

    def corner_send(n, i, p):
        return line_copies(n, i, p, down_recv, down_scale, down_sem, n, above)

    def middle_send(n, i, p):
        slot, target = MIDDLE_ROUTE[n]
        return line_copies(n, i, p, up_recv, up_scale, up_sem, slot, (beyond, below, above)[target])

    def corner_send_z(n, i):
        return line_z_copies(n, i, down_z, down_z_scale, down_z_sem, n, above)

    def middle_send_z(n, i):
        slot, target = MIDDLE_ROUTE[n]
        return line_z_copies(n, i, up_z, up_z_scale, up_z_sem, slot, (beyond, below, above)[target])

    def cross_copies(i):
        return (
            remote(
                cross_send_scale.at[i], cross_recv_scale.at[i],
                cross_send_sem.at[0], cross_recv_sem.at[i], across,
            ),
            remote(
                cross_send.at[i], cross_recv.at[i],
                cross_send_sem.at[1], cross_recv_sem.at[i], across,
            ),
        )

    def lanes_of(h):
        return slice(cuts[h][0], cuts[h][1] if h > 0 else width)

    def weighted_copy(h):
        at = lanes_of(h)
        return remote(
            weighted_send.at[:, at], weighted_recv.at[:, at], weighted_sem.at[parts], weighted_sem.at[h], peer
        )

    def fresh_copy(h):
        at = lanes_of(h)
        return remote(fresh_send.at[:, at], fresh_recv.at[:, at], fresh_sem.at[parts], fresh_sem.at[h], peer)

    def start(copies):
        for copy in copies:
            copy.start()

    def arrived(sem, coded_rows, scale_rows=1):
        both = measure_buf.at[pl.ds(0, coded_rows // 2 + scale_rows)]
        pltpu.make_async_copy(both, both, sem).wait()

    state = []
    for n, (src, dst) in enumerate(
        (
            (params_in, params), (first_in, first), (second_in, second), (anchor_in, anchor), (momentum_in, momentum),
            (steps_in, steps_smem), (tokens_in, tokens_smem),
        )
    ):
        state.append(pltpu.make_async_copy(src, dst, state_sem.at[n]))
    cot_local = pltpu.make_async_copy(cotangent, cot_buf.at[pl.ds(0, tokens)], cot_sem.at[0])
    cot_remote = pltpu.make_async_remote_copy(
        src_ref=cotangent,
        dst_ref=cot_buf.at[pl.ds(tokens, tokens)],
        send_sem=cot_sem.at[1],
        recv_sem=cot_sem.at[2],
        device_id=sibling,
        device_id_type=MESH,
    )

    barrier = pltpu.get_barrier_semaphore()
    for target in (sibling, across, above, peer):
        pl.semaphore_signal(barrier, inc=1, device_id=target, device_id_type=MESH)

    @pl.when(middle)
    def _():
        pl.semaphore_signal(barrier, inc=1, device_id=below, device_id_type=MESH)

    cot_local.start()
    for n in range(2):
        for far in (1, 0):
            acts_local(n, 0, far).start()
    cot_local.wait()
    cot_t[:, 0:tokens] = cot_buf[0:tokens].astype(jnp.float32).T.astype(jnp.bfloat16)
    pl.semaphore_wait(barrier, jnp.where(middle, 5, 4))
    cot_remote.start()
    for far in (1, 0):
        acts_remote(0, 0, far).start()

    @pl.when(middle)
    def _():
        pl.semaphore_signal(vouch_sem, inc=1, device_id=above, device_id_type=MESH)

    def encode(value):
        top = jnp.max(jnp.abs(value), axis=0, keepdims=True)
        levels = jnp.where(top > SMALLEST, LEVELS / jnp.maximum(top, SMALLEST), 0.0)
        return jnp.round(value * levels).astype(jnp.int32).astype(WIRE), top * (1.0 / LEVELS)

    def decode(coded, scale):
        return coded.astype(jnp.int32).astype(jnp.float32) * scale

    cot_remote.wait_recv()
    for far in (1, 0):
        acts_remote(1, 0, far).start()
    for n in range(2, LINE):
        fetch(n, 0)
    cot_t[:, tokens:] = cot_buf[tokens:].astype(jnp.float32).T.astype(jnp.bfloat16)

    def multiply(i):
        @pl.loop(0, LINE)
        def _(n):
            if i == 0:

                @pl.when(n >= LINE // 2)
                def _():
                    fetch(2 * n - LINE, 1)
                    fetch(2 * n - LINE + 1, 1)

            acts_arrived(n, i, 1)
            for p, (lo, hi) in enumerate(cuts):
                product = jnp.dot(cot_t[lanes_of(p)], acts_buf[i, n, 1], preferred_element_type=jnp.float32)
                x_send[n, i, lo:hi], x_send_scale[n, i, p] = encode(product[: hi - lo])
                if p == 0:
                    far_z[n, i] = product[hi - lo :]
            if i == 0:
                for p in range(parts):
                    start(x_copies(n, i, p))
            acts_arrived(n, i, 0)
            for p in range(parts):
                at = lanes_of(p)
                own[n, i, at] = jnp.dot(cot_t[at], acts_buf[i, n, 0], preferred_element_type=jnp.float32)

            @pl.when((corner & (n < LINE - 1)) | (middle & (n == 1)))
            def _():
                zz_send[n, i, 0], zz_send_scale[n, i, 0] = encode(own[n, i, tail])
                zz_send[n, i, 1], zz_send_scale[n, i, 1] = encode(far_z[n, i])

            @pl.when(corner & (n < LINE - 1))
            def _():
                start(corner_send_z(n, i))

            @pl.when(middle & (n == 1))
            def _():
                start(middle_send_z(1, i))

    def received(n, i, p):
        lo, hi = cuts[p]
        arrived(x_recv_sem.at[n, i, p], hi - lo)
        return own[n, i, lo:hi] + decode(x_recv[n, i, lo:hi], x_recv_scale[n, i, p])

    def plus_line(total, i, p, into, scale, sem, slot):
        lo, hi = cuts[p]
        arrived(sem.at[slot, i, p], hi - lo)
        return total + decode(into[slot, i, lo:hi], scale[slot, i, p])

    def plus_below(total, i, p, slot):
        return plus_line(total, i, p, down_recv, down_scale, down_sem, slot)

    def plus_above(total, i, p, slot):
        return plus_line(total, i, p, up_recv, up_scale, up_sem, slot)

    def hand_on(role, n, i, p):
        lo, hi = cuts[p]
        total = received(n, i, p)
        if role == "middle" and n != 1:
            total = plus_below(total, i, p, n // 2)
        z_send[n, i, lo:hi], z_send_scale[n, i, p] = encode(total)
        start(corner_send(n, i, p) if role == "corner" else middle_send(n, i, p))

    def line_z(n, i, above_slots, below_slots):
        streams = [(up_z, up_z_scale, up_z_sem, slot) for slot in above_slots]
        streams += [(down_z, down_z_scale, down_z_sem, slot) for slot in below_slots]
        totals = [own[n, i, tail], far_z[n, i]]
        for into, scale, sem, slot in streams:
            arrived(sem.at[slot, i], 2 * line_width, 2)
            totals = [totals[far] + decode(into[slot, i, far], scale[slot, i, far]) for far in range(2)]
        return totals

    def hand_on_z(n, i):
        totals = line_z(n, i, (), (n // 2,))
        for far in range(2):
            zz_send[n, i, far], zz_send_scale[n, i, far] = encode(totals[far])
        start(middle_send_z(n, i))

    def cross_over(role, i):
        totals = line_z(3, i, (0, 1), ()) if role == "corner" else line_z(3, i, (1,), (2,))
        cross_send[i], cross_send_scale[i] = encode(totals[1])
        start(cross_copies(i))
        own[3, i, tail] = totals[0]

    def correction(beta):
        count = jnp.full((1, 1), steps_smem[group], jnp.int32).astype(jnp.float32)
        return 1.0 - jnp.exp(count * float(np.log(np.float64(np.float32(beta)))))

    def share_of(at):
        return jnp.full((1, 1), tokens_smem[at], jnp.int32).astype(jnp.float32)

    def finish(role, i, h):
        total = received(3, i, h)
        if role == "corner":
            total = plus_above(total, i, h, 0)
            total = plus_above(total, i, h, 1)
        else:
            total = plus_above(total, i, h, 1)
            total = plus_below(total, i, h, 2)
        if h == 0:
            arrived(cross_recv_sem.at[i], line_width)
            total = jnp.concatenate([total, own[3, i, tail] + decode(cross_recv[i], cross_recv_scale[i])], axis=0)
        lanes = lanes_of(h)
        gradient = total.T / group_total
        at = pl.ds(pl.multiple_of(half_of(i) * half, half), half)
        weights = params[at, lanes]
        fresh_first = beta_one * first[at, lanes] + (1.0 - beta_one) * gradient
        fresh_second = beta_two * second[at, lanes] + (1.0 - beta_two) * gradient * gradient
        ratio = fresh_first / correction(beta_one) / (jnp.sqrt(fresh_second / correction(beta_two)) + epsilon)
        share = share_of(group) / (share_of(0) + share_of(1))
        weighted = share * (weights - inner_rate * (ratio + decay_rate * weights))
        if i == 0:
            weighted_send[:, lanes] = weighted
            weighted_copy(h).start()
            return
        weighted_copy(h).wait_recv()
        new_anchor, new_momentum = outer_update(anchor[:, lanes], momentum[:, lanes], weighted + weighted_recv[:, lanes])
        rounded = new_anchor.astype(jnp.bfloat16)
        fresh_send[:, lanes] = rounded
        fresh_copy(h).start()
        anchor_out[:, lanes] = new_anchor
        momentum_out[:, lanes] = new_momentum
        weights_out[at, lanes] = rounded

    def run(role, plan):
        for event in plan:
            kind, rest = event[0], event[1:]
            if kind == "pass":
                for p in range(parts):
                    hand_on(role, *rest, p)
            elif kind == "pass_z":
                hand_on_z(*rest)
            elif kind == "cross":
                cross_over(role, *rest)
            elif kind == "start_x":
                for n in range(*rest[1:]):
                    for p in range(parts):
                        start(x_copies(n, rest[0], p))
            else:
                for h in range(parts):
                    finish(role, *rest, h)

    multiply(0)
    for copy in state:
        copy.start()

    @pl.when(corner)
    def _():
        run("corner", (("pass", 0, 0),))

    @pl.when(middle)
    def _():
        pl.semaphore_wait(vouch_sem, 1)
        run("middle", (("pass_z", 0, 0),))

    multiply(1)
    for copy in state:
        copy.wait()

    @pl.when(corner)
    def _():
        run("corner", CORNER_PLAN)

    @pl.when(middle)
    def _():
        run("middle", MIDDLE_PLAN)

    theirs = pl.ds(pl.multiple_of(other_group * half, half), half)
    for h in range(parts):
        fresh_copy(h).wait_recv()
        weights_out[theirs, lanes_of(h)] = fresh_recv[:, lanes_of(h)]

    cot_remote.wait_send()
    remote(acts_buf.at[0], acts_buf.at[0], acts_send_sem, acts_send_sem, sibling).wait_send()
    for buffer, sem in (
        (x_send_scale, x_send_sem.at[0]),
        (x_send, x_send_sem.at[1]),
        (z_send_scale, z_send_sem.at[0]),
        (z_send, z_send_sem.at[1]),
        (zz_send_scale, zz_send_sem.at[0]),
        (zz_send, zz_send_sem.at[1]),
        (cross_send_scale, cross_send_sem.at[0]),
        (cross_send, cross_send_sem.at[1]),
        (weighted_send, weighted_sem.at[parts]),
        (fresh_send, fresh_sem.at[parts]),
    ):
        remote(buffer, buffer, sem, sem, sibling).wait_send()


def write_out_kernel(anchor, momentum, weights, anchor_out, momentum_out, weights_out, sem):
    copies = [
        pltpu.make_async_copy(src, dst, sem.at[n])
        for n, (src, dst) in enumerate(((anchor, anchor_out), (momentum, momentum_out), (weights, weights_out)))
    ]
    for copy in copies:
        copy.start()
    for copy in copies:
        copy.wait()


def fused_per_device(
    acts, cotangent, inner_params, adam_first, adam_second, inner_steps, group_tokens, anchor, momentum
):
    tokens, _ = acts.shape[1:]
    rows, width = inner_params.shape[1:]
    half, line_width = rows // 2, line_width_of(width)
    low, full = jnp.bfloat16, jnp.float32
    dma = pltpu.SemaphoreType.DMA
    vmem = pltpu.VMEM
    body = width - line_width
    parts = len(cuts_of(width))
    operands = (
        inner_steps, group_tokens, acts[0], cotangent[0], inner_params[0], adam_first[0], adam_second[0],
        anchor, momentum,
    )
    results = pl.pallas_call(
        functools.partial(outer_step_kernel, tokens * lax.axis_size("fsdp")),
        out_shape=(
            vmem(anchor.shape, full),
            vmem(anchor.shape, full),
            vmem((rows, width), low),
        ),
        in_specs=[pl.BlockSpec(memory_space=pltpu.HBM)] * 9,
        out_specs=[pl.BlockSpec(memory_space=pltpu.VMEM)] * 3,
        scratch_shapes=[
            pltpu.SMEM(inner_steps.shape, jnp.int32),
            pltpu.SMEM(group_tokens.shape, jnp.int32),
            vmem((2, LINE, 2, 2 * tokens, half), low),
            vmem((2 * tokens, width), low),
            vmem((width, 2 * tokens), low),
            vmem((LINE, 2, width, half), full),
            vmem((LINE, 2, line_width, half), full),
            vmem((LINE, 2, body, half), WIRE),
            vmem((LINE, 2, body, half), WIRE),
            vmem((LINE, 2, parts, 1, half), full),
            vmem((LINE, 2, parts, 1, half), full),
            vmem((3, 2, body, half), WIRE),
            vmem((3, 2, parts, 1, half), full),
            vmem((3, 2, body, half), WIRE),
            vmem((3, 2, parts, 1, half), full),
            vmem((2, 2, body, half), WIRE),
            vmem((2, 2, parts, 1, half), full),
            vmem((3, 2, 2, line_width, half), WIRE),
            vmem((3, 2, 2, 1, half), full),
            vmem((3, 2, 2, line_width, half), WIRE),
            vmem((3, 2, 2, 1, half), full),
            vmem((2, 2, 2, line_width, half), WIRE),
            vmem((2, 2, 2, 1, half), full),
            vmem((2, line_width, half), WIRE),
            vmem((2, line_width, half), WIRE),
            vmem((2, 1, half), full),
            vmem((2, 1, half), full),
            *[vmem((rows, width), full)] * 3,
            *[vmem((half, width), full)] * 2,
            *[vmem((half, width), full)] * 2,
            *[vmem((half, width), low)] * 2,
            vmem((max(width // 8, line_width) + 2, 1, half), full),
            pltpu.SemaphoreType.REGULAR,
            dma,
            dma((2, LINE, 2)),
            dma((3,)),
            dma((7,)),
            dma((2,)),
            dma((LINE, 2, parts)),
            dma((2,)),
            dma((3, 2, parts)),
            dma((2, 2, parts)),
            dma((2,)),
            dma((3, 2)),
            dma((2, 2)),
            dma((2,)),
            dma((2,)),
            dma((parts + 1,)),
            dma((parts + 1,)),
        ],
        compiler_params=pltpu.CompilerParams(
            collective_id=0, has_side_effects=True, vmem_limit_bytes=48 * 1024 * 1024
        ),
    )(*(pltpu.with_memory_space_constraint(operand, pltpu.HBM) for operand in operands))
    new_anchor, new_momentum, weights = pl.pallas_call(
        write_out_kernel,
        out_shape=(
            jax.ShapeDtypeStruct(anchor.shape, full),
            jax.ShapeDtypeStruct(anchor.shape, full),
            jax.ShapeDtypeStruct((rows, width), low),
        ),
        in_specs=[pl.BlockSpec(memory_space=pltpu.VMEM)] * 3,
        out_specs=[pl.BlockSpec(memory_space=pl.ANY)] * 3,
        scratch_shapes=[dma((3,))],
        compiler_params=pltpu.CompilerParams(vmem_limit_bytes=4 * 1024 * 1024),
    )(*results)
    return (new_anchor, new_momentum, weights[None])


def choose(*arguments):
    rows, width = arguments[2].shape[1:]
    fits = lax.axis_size("fsdp") == FSDP and lax.axis_size("group") == GROUPS
    if fits and rows % 256 == 0 and width % 512 == 0:
        return fused_per_device(*arguments)
    return per_device(*arguments)


def solution(mesh):
    placed = (
        P("group", "fsdp", None),
        P("group", "fsdp", None),
        P("group", "fsdp", None),
        P("group", "fsdp", None),
        P("group", "fsdp", None),
        P(),
        P(),
        P(("fsdp", "group"), None),
        P(("fsdp", "group"), None),
    )
    return jax.shard_map(
        choose,
        mesh=mesh,
        in_specs=placed,
        out_specs=(
            P(("fsdp", "group"), None),
            P(("fsdp", "group"), None),
            P("group", "fsdp", None),
        ),
        check_vma=False,
    )
```

```python
import functools

import jax
import jax.numpy as jnp
import numpy as np
from jax import lax
from jax.experimental import pallas as pl
from jax.experimental.pallas import tpu as pltpu
from jax.sharding import PartitionSpec as P

beta_one = 0.9
beta_two = 0.95
epsilon = 1e-08
inner_rate = 0.3
decay_rate = 0.1
outer_rate = 0.7
outer_mom = 0.9


def inner_update(params, first_moment, second_moment, gradient, steps):
    fresh_first = beta_one * first_moment + (1.0 - beta_one) * gradient
    fresh_second = beta_two * second_moment + (1.0 - beta_two) * gradient * gradient
    steps_float = steps.astype(jnp.float32)
    correct_one = 1.0 - jnp.power(jnp.float32(beta_one), steps_float)
    correct_two = 1.0 - jnp.power(jnp.float32(beta_two), steps_float)
    ratio = fresh_first / correct_one / (jnp.sqrt(fresh_second / correct_two) + epsilon)
    return params - inner_rate * (ratio + decay_rate * params)


def outer_update(anchor, momentum, merged):
    pseudo = anchor - merged
    fresh_momentum = outer_mom * momentum + pseudo
    fresh_anchor = anchor - outer_rate * (pseudo + outer_mom * fresh_momentum)
    return (fresh_anchor, fresh_momentum)


def per_device(
    acts,
    cotangent,
    inner_params,
    adam_first,
    adam_second,
    inner_steps,
    group_tokens,
    anchor,
    momentum,
):
    fsdp_count = lax.axis_size("fsdp")
    group_index = lax.axis_index("group")
    inputs = acts[0]
    upstream = cotangent[0]
    group_total = inputs.shape[0] * fsdp_count
    contract = (((0,), (0,)), ((), ()))
    summed = lax.psum_scatter(
        lax.dot_general(inputs, upstream, contract, preferred_element_type=jnp.float32),
        "fsdp",
        scatter_dimension=0,
        tiled=True,
    )
    gradient = summed / group_total
    steps = lax.dynamic_index_in_dim(inner_steps, group_index, 0, False)
    updated = inner_update(inner_params[0], adam_first[0], adam_second[0], gradient, steps)
    counts = group_tokens.astype(jnp.float32)
    share = lax.dynamic_index_in_dim(counts, group_index, 0, False) / jnp.sum(counts)
    weighted = share * updated
    merged = lax.psum_scatter(weighted, "group", scatter_dimension=0, tiled=True)
    new_anchor, new_momentum = outer_update(anchor, momentum, merged)
    rebuilt = lax.all_gather(new_anchor.astype(jnp.bfloat16), "group", axis=0, tiled=True)
    return (new_anchor, new_momentum, rebuilt[None])


MESH = pl.DeviceIdType.MESH
WIRE = jnp.int16
LEVELS = 32767.0
SMALLEST = 1e-30
LINE = 4
FSDP = 16
GROUPS = 2
MIDDLE_ROUTE = ((1, 0), (0, 1), (1, 2))
CORNER_PLAN = (
    ("pass", 1, 0), ("cross", 0), ("start_x", 1, 0, 3), ("pass", 2, 0),
    ("cross", 1), ("start_x", 1, 3, 4), ("pass", 0, 1), ("finish", 0), ("pass", 1, 1), ("pass", 2, 1), ("finish", 1),
)
MIDDLE_PLAN = (
    ("pass_z", 2, 0), ("pass", 0, 0), ("pass", 1, 0), ("cross", 0), ("start_x", 1, 0, 3), ("pass_z", 0, 1),
    ("pass_z", 2, 1), ("pass", 2, 0), ("cross", 1), ("start_x", 1, 3, 4), ("finish", 0),
    ("pass", 1, 1), ("pass", 0, 1), ("pass", 2, 1), ("finish", 1),
)


def line_width_of(width):
    return width // 16 * 6 // 32 * 16


def cuts_of(width):
    step, last = width // 4, width - line_width_of(width)
    cuts = [(lo, min(lo + step, last)) for lo in range(0, last, step)]
    return (cuts[-1], *cuts[:-1])


def outer_step_kernel(
    group_total,
    steps_in,
    tokens_in,
    acts,
    cotangent,
    params_in,
    first_in,
    second_in,
    anchor_in,
    momentum_in,
    anchor_out,
    momentum_out,
    weights_out,
    steps_smem,
    tokens_smem,
    acts_buf,
    cot_buf,
    cot_t,
    own,
    far_z,
    x_send,
    x_recv,
    x_send_scale,
    x_recv_scale,
    z_send,
    z_send_scale,
    down_recv,
    down_scale,
    up_recv,
    up_scale,
    zz_send,
    zz_send_scale,
    down_z,
    down_z_scale,
    up_z,
    up_z_scale,
    cross_send,
    cross_recv,
    cross_send_scale,
    cross_recv_scale,
    params,
    first,
    second,
    anchor,
    momentum,
    weighted_send,
    weighted_recv,
    fresh_send,
    fresh_recv,
    measure_buf,
    vouch_sem,
    acts_send_sem,
    acts_recv_sem,
    cot_sem,
    state_sem,
    x_send_sem,
    x_recv_sem,
    z_send_sem,
    down_sem,
    up_sem,
    zz_send_sem,
    down_z_sem,
    up_z_sem,
    cross_send_sem,
    cross_recv_sem,
    weighted_sem,
    fresh_sem,
):
    tokens, _ = acts.shape
    rows, width = params.shape
    half = rows // 2
    line_width = line_width_of(width)
    cuts = cuts_of(width)
    parts = len(cuts)
    tail = slice(width - line_width, width)
    me = lax.axis_index("fsdp")
    group = lax.axis_index("group")
    other_group = 1 - group
    core, x, z = me % 2, (me // 2) % 2, me // 4
    lower = z < 2
    corner = (z == 0) | (z == LINE - 1)
    middle = jnp.logical_not(corner)
    toward = jnp.where(lower, 1, -1)

    sibling = (group, me + 1 - 2 * core)
    across = (group, me + 2 - 4 * x)
    above = (group, me + 4 * toward)
    below = (group, me - 4 * toward)
    beyond = (group, me + 8 * toward)
    peer = (other_group, me)

    def place(n):
        mid = jnp.where(n == 0, 3, jnp.where(n == 1, 0, jnp.where(n == 2, 2, 1)))
        level = jnp.where(corner, 3 - n, mid)
        return jnp.where(lower, level, 3 - level)

    def half_of(i):
        return (other_group + i) % 2

    def columns(n, far, i, owner_core):
        owner_x = jnp.where(far == 1, 1 - x, x)
        block = (place(n) * 2 + owner_x) * 2 + owner_core
        return pl.ds(pl.multiple_of(block * rows + half_of(i) * half, half), half)

    def acts_local(n, i, far):
        return pltpu.make_async_copy(
            acts.at[:, columns(n, far, i, core)],
            acts_buf.at[i, n, far, pl.ds(0, tokens)],
            acts_recv_sem.at[i, n, far],
        )

    def acts_remote(n, i, far):
        return pltpu.make_async_remote_copy(
            src_ref=acts.at[:, columns(n, far, i, 1 - core)],
            dst_ref=acts_buf.at[i, n, far, pl.ds(tokens, tokens)],
            send_sem=acts_send_sem,
            recv_sem=acts_recv_sem.at[i, n, far],
            device_id=sibling,
            device_id_type=MESH,
        )

    def acts_arrived(n, i, far):
        whole = acts_buf.at[i, n, far]
        pltpu.make_async_copy(whole, whole, acts_recv_sem.at[i, n, far]).wait()

    def fetch(n, i):
        for far in (1, 0):
            acts_local(n, i, far).start()
            acts_remote(n, i, far).start()

    def remote(src, dst, send_sem, recv_sem, target):
        return pltpu.make_async_remote_copy(
            src_ref=src, dst_ref=dst, send_sem=send_sem, recv_sem=recv_sem, device_id=target, device_id_type=MESH
        )

    def x_copies(n, i, p):
        lo, hi = cuts[p]
        return (
            remote(
                x_send_scale.at[n, i, p], x_recv_scale.at[n, i, p],
                x_send_sem.at[0], x_recv_sem.at[n, i, p], across,
            ),
            remote(
                x_send.at[n, i, pl.ds(lo, hi - lo)], x_recv.at[n, i, pl.ds(lo, hi - lo)],
                x_send_sem.at[1], x_recv_sem.at[n, i, p], across,
            ),
        )

    def line_copies(n, i, p, into, scale, sem, slot, target):
        lo, hi = cuts[p]
        return (
            remote(
                z_send_scale.at[n, i, p], scale.at[slot, i, p],
                z_send_sem.at[0], sem.at[slot, i, p], target,
            ),
            remote(
                z_send.at[n, i, pl.ds(lo, hi - lo)], into.at[slot, i, pl.ds(lo, hi - lo)],
                z_send_sem.at[1], sem.at[slot, i, p], target,
            ),
        )

    def line_z_copies(n, i, into, scale, sem, slot, target):
        return (
            remote(
                zz_send_scale.at[n, i], scale.at[slot, i],
                zz_send_sem.at[0], sem.at[slot, i], target,
            ),
            remote(
                zz_send.at[n, i], into.at[slot, i],
                zz_send_sem.at[1], sem.at[slot, i], target,
            ),
        )

    def corner_send(n, i, p):
        return line_copies(n, i, p, down_recv, down_scale, down_sem, n, above)

    def middle_send(n, i, p):
        slot, target = MIDDLE_ROUTE[n]
        return line_copies(n, i, p, up_recv, up_scale, up_sem, slot, (beyond, below, above)[target])

    def corner_send_z(n, i):
        return line_z_copies(n, i, down_z, down_z_scale, down_z_sem, n, above)

    def middle_send_z(n, i):
        slot, target = MIDDLE_ROUTE[n]
        return line_z_copies(n, i, up_z, up_z_scale, up_z_sem, slot, (beyond, below, above)[target])

    def cross_copies(i):
        return (
            remote(
                cross_send_scale.at[i], cross_recv_scale.at[i],
                cross_send_sem.at[0], cross_recv_sem.at[i], across,
            ),
            remote(
                cross_send.at[i], cross_recv.at[i],
                cross_send_sem.at[1], cross_recv_sem.at[i], across,
            ),
        )

    def lanes_of(h):
        return slice(cuts[h][0], cuts[h][1] if h > 0 else width)

    def weighted_copy(h):
        at = lanes_of(h)
        return remote(
            weighted_send.at[:, at], weighted_recv.at[:, at], weighted_sem.at[parts], weighted_sem.at[h], peer
        )

    def fresh_copy(h):
        at = lanes_of(h)
        return remote(fresh_send.at[:, at], fresh_recv.at[:, at], fresh_sem.at[parts], fresh_sem.at[h], peer)

    def start(copies):
        for copy in copies:
            copy.start()

    def arrived(sem, coded_rows, scale_rows=1):
        both = measure_buf.at[pl.ds(0, coded_rows // 2 + scale_rows)]
        pltpu.make_async_copy(both, both, sem).wait()

    state = []
    for n, (src, dst) in enumerate(
        (
            (params_in, params), (first_in, first), (second_in, second), (anchor_in, anchor), (momentum_in, momentum),
            (steps_in, steps_smem), (tokens_in, tokens_smem),
        )
    ):
        state.append(pltpu.make_async_copy(src, dst, state_sem.at[n]))
    cot_local = pltpu.make_async_copy(cotangent, cot_buf.at[pl.ds(0, tokens)], cot_sem.at[0])
    cot_remote = pltpu.make_async_remote_copy(
        src_ref=cotangent,
        dst_ref=cot_buf.at[pl.ds(tokens, tokens)],
        send_sem=cot_sem.at[1],
        recv_sem=cot_sem.at[2],
        device_id=sibling,
        device_id_type=MESH,
    )

    barrier = pltpu.get_barrier_semaphore()
    for target in (sibling, across, above, peer):
        pl.semaphore_signal(barrier, inc=1, device_id=target, device_id_type=MESH)

    @pl.when(middle)
    def _():
        pl.semaphore_signal(barrier, inc=1, device_id=below, device_id_type=MESH)

    cot_local.start()
    for n in range(2):
        for far in (1, 0):
            acts_local(n, 0, far).start()
    pl.semaphore_wait(barrier, jnp.where(middle, 5, 4))
    cot_remote.start()
    for far in (1, 0):
        acts_remote(0, 0, far).start()
    for far in (1, 0):
        acts_remote(1, 0, far).start()

    @pl.when(middle)
    def _():
        pl.semaphore_signal(vouch_sem, inc=1, device_id=above, device_id_type=MESH)

    def encode(value):
        top = jnp.max(jnp.abs(value), axis=0, keepdims=True)
        levels = jnp.where(top > SMALLEST, LEVELS / jnp.maximum(top, SMALLEST), 0.0)
        return jnp.round(value * levels).astype(jnp.int32).astype(WIRE), top * (1.0 / LEVELS)

    def decode(coded, scale):
        return coded.astype(jnp.int32).astype(jnp.float32) * scale

    cot_local.wait()
    cot_t[:, 0:tokens] = cot_buf[0:tokens].astype(jnp.float32).T.astype(jnp.bfloat16)
    cot_remote.wait_recv()
    for n in range(2, LINE):
        fetch(n, 0)
    cot_t[:, tokens:] = cot_buf[tokens:].astype(jnp.float32).T.astype(jnp.bfloat16)

    def multiply(i):
        @pl.loop(0, LINE)
        def _(n):
            if i == 0:

                @pl.when(n >= LINE // 2)
                def _():
                    fetch(2 * n - LINE, 1)
                    fetch(2 * n - LINE + 1, 1)

            acts_arrived(n, i, 1)
            for p, (lo, hi) in enumerate(cuts):
                product = jnp.dot(cot_t[lanes_of(p)], acts_buf[i, n, 1], preferred_element_type=jnp.float32)
                x_send[n, i, lo:hi], x_send_scale[n, i, p] = encode(product[: hi - lo])
                if p == 0:
                    far_z[n, i] = product[hi - lo :]
            if i == 0:
                for p in range(parts):
                    start(x_copies(n, i, p))
            acts_arrived(n, i, 0)
            for p in range(parts):
                at = lanes_of(p)
                own[n, i, at] = jnp.dot(cot_t[at], acts_buf[i, n, 0], preferred_element_type=jnp.float32)

            @pl.when((corner & (n < LINE - 1)) | (middle & (n == 1)))
            def _():
                zz_send[n, i, 0], zz_send_scale[n, i, 0] = encode(own[n, i, tail])
                zz_send[n, i, 1], zz_send_scale[n, i, 1] = encode(far_z[n, i])

            @pl.when(corner & (n < LINE - 1))
            def _():
                start(corner_send_z(n, i))

            @pl.when(middle & (n == 1))
            def _():
                start(middle_send_z(1, i))

    def received(n, i, p):
        lo, hi = cuts[p]
        arrived(x_recv_sem.at[n, i, p], hi - lo)
        return own[n, i, lo:hi] + decode(x_recv[n, i, lo:hi], x_recv_scale[n, i, p])

    def plus_line(total, i, p, into, scale, sem, slot):
        lo, hi = cuts[p]
        arrived(sem.at[slot, i, p], hi - lo)
        return total + decode(into[slot, i, lo:hi], scale[slot, i, p])

    def plus_below(total, i, p, slot):
        return plus_line(total, i, p, down_recv, down_scale, down_sem, slot)

    def plus_above(total, i, p, slot):
        return plus_line(total, i, p, up_recv, up_scale, up_sem, slot)

    def hand_on(role, n, i, p):
        lo, hi = cuts[p]
        total = received(n, i, p)
        if role == "middle" and n != 1:
            total = plus_below(total, i, p, n // 2)
        z_send[n, i, lo:hi], z_send_scale[n, i, p] = encode(total)
        start(corner_send(n, i, p) if role == "corner" else middle_send(n, i, p))

    def line_z(n, i, above_slots, below_slots):
        streams = [(up_z, up_z_scale, up_z_sem, slot) for slot in above_slots]
        streams += [(down_z, down_z_scale, down_z_sem, slot) for slot in below_slots]
        totals = [own[n, i, tail], far_z[n, i]]
        for into, scale, sem, slot in streams:
            arrived(sem.at[slot, i], 2 * line_width, 2)
            totals = [totals[far] + decode(into[slot, i, far], scale[slot, i, far]) for far in range(2)]
        return totals

    def hand_on_z(n, i):
        totals = line_z(n, i, (), (n // 2,))
        for far in range(2):
            zz_send[n, i, far], zz_send_scale[n, i, far] = encode(totals[far])
        start(middle_send_z(n, i))

    def cross_over(role, i):
        totals = line_z(3, i, (0, 1), ()) if role == "corner" else line_z(3, i, (1,), (2,))
        cross_send[i], cross_send_scale[i] = encode(totals[1])
        start(cross_copies(i))
        own[3, i, tail] = totals[0]

    def correction(beta):
        count = jnp.full((1, 1), steps_smem[group], jnp.int32).astype(jnp.float32)
        return 1.0 - jnp.exp(count * float(np.log(np.float64(np.float32(beta)))))

    def share_of(at):
        return jnp.full((1, 1), tokens_smem[at], jnp.int32).astype(jnp.float32)

    def finish(role, i, h):
        total = received(3, i, h)
        if role == "corner":
            total = plus_above(total, i, h, 0)
            total = plus_above(total, i, h, 1)
        else:
            total = plus_above(total, i, h, 1)
            total = plus_below(total, i, h, 2)
        if h == 0:
            arrived(cross_recv_sem.at[i], line_width)
            total = jnp.concatenate([total, own[3, i, tail] + decode(cross_recv[i], cross_recv_scale[i])], axis=0)
        lanes = lanes_of(h)
        gradient = total.T / group_total
        at = pl.ds(pl.multiple_of(half_of(i) * half, half), half)
        weights = params[at, lanes]
        fresh_first = beta_one * first[at, lanes] + (1.0 - beta_one) * gradient
        fresh_second = beta_two * second[at, lanes] + (1.0 - beta_two) * gradient * gradient
        ratio = fresh_first / correction(beta_one) / (jnp.sqrt(fresh_second / correction(beta_two)) + epsilon)
        share = share_of(group) / (share_of(0) + share_of(1))
        weighted = share * (weights - inner_rate * (ratio + decay_rate * weights))
        if i == 0:
            weighted_send[:, lanes] = weighted
            weighted_copy(h).start()
            return
        weighted_copy(h).wait_recv()
        new_anchor, new_momentum = outer_update(anchor[:, lanes], momentum[:, lanes], weighted + weighted_recv[:, lanes])
        rounded = new_anchor.astype(jnp.bfloat16)
        fresh_send[:, lanes] = rounded
        fresh_copy(h).start()
        anchor_out[:, lanes] = new_anchor
        momentum_out[:, lanes] = new_momentum
        weights_out[at, lanes] = rounded

    def run(role, plan):
        for event in plan:
            kind, rest = event[0], event[1:]
            if kind == "pass":
                for p in range(parts):
                    hand_on(role, *rest, p)
            elif kind == "pass_z":
                hand_on_z(*rest)
            elif kind == "cross":
                cross_over(role, *rest)
            elif kind == "start_x":
                for n in range(*rest[1:]):
                    for p in range(parts):
                        start(x_copies(n, rest[0], p))
            else:
                for h in range(parts):
                    finish(role, *rest, h)

    multiply(0)
    for copy in state:
        copy.start()

    @pl.when(corner)
    def _():
        run("corner", (("pass", 0, 0),))

    @pl.when(middle)
    def _():
        pl.semaphore_wait(vouch_sem, 1)
        run("middle", (("pass_z", 0, 0),))

    multiply(1)
    for copy in state:
        copy.wait()

    @pl.when(corner)
    def _():
        run("corner", CORNER_PLAN)

    @pl.when(middle)
    def _():
        run("middle", MIDDLE_PLAN)

    theirs = pl.ds(pl.multiple_of(other_group * half, half), half)
    for h in range(parts):
        fresh_copy(h).wait_recv()
        weights_out[theirs, lanes_of(h)] = fresh_recv[:, lanes_of(h)]

    cot_remote.wait_send()
    remote(acts_buf.at[0], acts_buf.at[0], acts_send_sem, acts_send_sem, sibling).wait_send()
    for buffer, sem in (
        (x_send_scale, x_send_sem.at[0]),
        (x_send, x_send_sem.at[1]),
        (z_send_scale, z_send_sem.at[0]),
        (z_send, z_send_sem.at[1]),
        (zz_send_scale, zz_send_sem.at[0]),
        (zz_send, zz_send_sem.at[1]),
        (cross_send_scale, cross_send_sem.at[0]),
        (cross_send, cross_send_sem.at[1]),
        (weighted_send, weighted_sem.at[parts]),
        (fresh_send, fresh_sem.at[parts]),
    ):
        remote(buffer, buffer, sem, sem, sibling).wait_send()


def write_out_kernel(anchor, momentum, weights, anchor_out, momentum_out, weights_out, sem):
    copies = [
        pltpu.make_async_copy(src, dst, sem.at[n])
        for n, (src, dst) in enumerate(((anchor, anchor_out), (momentum, momentum_out), (weights, weights_out)))
    ]
    for copy in copies:
        copy.start()
    for copy in copies:
        copy.wait()


def fused_per_device(
    acts, cotangent, inner_params, adam_first, adam_second, inner_steps, group_tokens, anchor, momentum
):
    tokens, _ = acts.shape[1:]
    rows, width = inner_params.shape[1:]
    half, line_width = rows // 2, line_width_of(width)
    low, full = jnp.bfloat16, jnp.float32
    dma = pltpu.SemaphoreType.DMA
    vmem = pltpu.VMEM
    body = width - line_width
    parts = len(cuts_of(width))
    operands = (
        inner_steps, group_tokens, acts[0], cotangent[0], inner_params[0], adam_first[0], adam_second[0],
        anchor, momentum,
    )
    results = pl.pallas_call(
        functools.partial(outer_step_kernel, tokens * lax.axis_size("fsdp")),
        out_shape=(
            vmem(anchor.shape, full),
            vmem(anchor.shape, full),
            vmem((rows, width), low),
        ),
        in_specs=[pl.BlockSpec(memory_space=pltpu.HBM)] * 9,
        out_specs=[pl.BlockSpec(memory_space=pltpu.VMEM)] * 3,
        scratch_shapes=[
            pltpu.SMEM(inner_steps.shape, jnp.int32),
            pltpu.SMEM(group_tokens.shape, jnp.int32),
            vmem((2, LINE, 2, 2 * tokens, half), low),
            vmem((2 * tokens, width), low),
            vmem((width, 2 * tokens), low),
            vmem((LINE, 2, width, half), full),
            vmem((LINE, 2, line_width, half), full),
            vmem((LINE, 2, body, half), WIRE),
            vmem((LINE, 2, body, half), WIRE),
            vmem((LINE, 2, parts, 1, half), full),
            vmem((LINE, 2, parts, 1, half), full),
            vmem((3, 2, body, half), WIRE),
            vmem((3, 2, parts, 1, half), full),
            vmem((3, 2, body, half), WIRE),
            vmem((3, 2, parts, 1, half), full),
            vmem((2, 2, body, half), WIRE),
            vmem((2, 2, parts, 1, half), full),
            vmem((3, 2, 2, line_width, half), WIRE),
            vmem((3, 2, 2, 1, half), full),
            vmem((3, 2, 2, line_width, half), WIRE),
            vmem((3, 2, 2, 1, half), full),
            vmem((2, 2, 2, line_width, half), WIRE),
            vmem((2, 2, 2, 1, half), full),
            vmem((2, line_width, half), WIRE),
            vmem((2, line_width, half), WIRE),
            vmem((2, 1, half), full),
            vmem((2, 1, half), full),
            *[vmem((rows, width), full)] * 3,
            *[vmem((half, width), full)] * 2,
            *[vmem((half, width), full)] * 2,
            *[vmem((half, width), low)] * 2,
            vmem((max(width // 8, line_width) + 2, 1, half), full),
            pltpu.SemaphoreType.REGULAR,
            dma,
            dma((2, LINE, 2)),
            dma((3,)),
            dma((7,)),
            dma((2,)),
            dma((LINE, 2, parts)),
            dma((2,)),
            dma((3, 2, parts)),
            dma((2, 2, parts)),
            dma((2,)),
            dma((3, 2)),
            dma((2, 2)),
            dma((2,)),
            dma((2,)),
            dma((parts + 1,)),
            dma((parts + 1,)),
        ],
        compiler_params=pltpu.CompilerParams(
            collective_id=0, has_side_effects=True, vmem_limit_bytes=48 * 1024 * 1024
        ),
    )(*(pltpu.with_memory_space_constraint(operand, pltpu.HBM) for operand in operands))
    new_anchor, new_momentum, weights = pl.pallas_call(
        write_out_kernel,
        out_shape=(
            jax.ShapeDtypeStruct(anchor.shape, full),
            jax.ShapeDtypeStruct(anchor.shape, full),
            jax.ShapeDtypeStruct((rows, width), low),
        ),
        in_specs=[pl.BlockSpec(memory_space=pltpu.VMEM)] * 3,
        out_specs=[pl.BlockSpec(memory_space=pl.ANY)] * 3,
        scratch_shapes=[dma((3,))],
        compiler_params=pltpu.CompilerParams(vmem_limit_bytes=4 * 1024 * 1024),
    )(*results)
    return (new_anchor, new_momentum, weights[None])


def choose(*arguments):
    rows, width = arguments[2].shape[1:]
    fits = lax.axis_size("fsdp") == FSDP and lax.axis_size("group") == GROUPS
    if fits and rows % 256 == 0 and width % 512 == 0:
        return fused_per_device(*arguments)
    return per_device(*arguments)


def solution(mesh):
    placed = (
        P("group", "fsdp", None),
        P("group", "fsdp", None),
        P("group", "fsdp", None),
        P("group", "fsdp", None),
        P("group", "fsdp", None),
        P(),
        P(),
        P(("fsdp", "group"), None),
        P(("fsdp", "group"), None),
    )
    return jax.shard_map(
        choose,
        mesh=mesh,
        in_specs=placed,
        out_specs=(
            P(("fsdp", "group"), None),
            P(("fsdp", "group"), None),
            P("group", "fsdp", None),
        ),
        check_vma=False,
    )
```

```python
import functools

import jax
import jax.numpy as jnp
import numpy as np
from jax import lax
from jax.experimental import pallas as pl
from jax.experimental.pallas import tpu as pltpu
from jax.sharding import PartitionSpec as P

beta_one = 0.9
beta_two = 0.95
epsilon = 1e-08
inner_rate = 0.3
decay_rate = 0.1
outer_rate = 0.7
outer_mom = 0.9


def inner_update(params, first_moment, second_moment, gradient, steps):
    fresh_first = beta_one * first_moment + (1.0 - beta_one) * gradient
    fresh_second = beta_two * second_moment + (1.0 - beta_two) * gradient * gradient
    steps_float = steps.astype(jnp.float32)
    correct_one = 1.0 - jnp.power(jnp.float32(beta_one), steps_float)
    correct_two = 1.0 - jnp.power(jnp.float32(beta_two), steps_float)
    ratio = fresh_first / correct_one / (jnp.sqrt(fresh_second / correct_two) + epsilon)
    return params - inner_rate * (ratio + decay_rate * params)


def outer_update(anchor, momentum, merged):
    pseudo = anchor - merged
    fresh_momentum = outer_mom * momentum + pseudo
    fresh_anchor = anchor - outer_rate * (pseudo + outer_mom * fresh_momentum)
    return (fresh_anchor, fresh_momentum)


def per_device(
    acts,
    cotangent,
    inner_params,
    adam_first,
    adam_second,
    inner_steps,
    group_tokens,
    anchor,
    momentum,
):
    fsdp_count = lax.axis_size("fsdp")
    group_index = lax.axis_index("group")
    inputs = acts[0]
    upstream = cotangent[0]
    group_total = inputs.shape[0] * fsdp_count
    contract = (((0,), (0,)), ((), ()))
    summed = lax.psum_scatter(
        lax.dot_general(inputs, upstream, contract, preferred_element_type=jnp.float32),
        "fsdp",
        scatter_dimension=0,
        tiled=True,
    )
    gradient = summed / group_total
    steps = lax.dynamic_index_in_dim(inner_steps, group_index, 0, False)
    updated = inner_update(inner_params[0], adam_first[0], adam_second[0], gradient, steps)
    counts = group_tokens.astype(jnp.float32)
    share = lax.dynamic_index_in_dim(counts, group_index, 0, False) / jnp.sum(counts)
    weighted = share * updated
    merged = lax.psum_scatter(weighted, "group", scatter_dimension=0, tiled=True)
    new_anchor, new_momentum = outer_update(anchor, momentum, merged)
    rebuilt = lax.all_gather(new_anchor.astype(jnp.bfloat16), "group", axis=0, tiled=True)
    return (new_anchor, new_momentum, rebuilt[None])


MESH = pl.DeviceIdType.MESH
WIRE = jnp.int16
LEVELS = 32767.0
SMALLEST = 1e-30
LINE = 4
FSDP = 16
GROUPS = 2
MIDDLE_ROUTE = ((1, 0), (0, 1), (1, 2))
CORNER_PLAN = (
    ("pass", 1, 0), ("cross", 0), ("start_x", 1, 0, 3), ("pass", 2, 0),
    ("cross", 1), ("start_x", 1, 3, 4), ("pass", 0, 1), ("finish", 0), ("pass", 1, 1), ("pass", 2, 1), ("finish", 1),
)
MIDDLE_PLAN = (
    ("pass_z", 2, 0), ("pass", 0, 0), ("pass", 1, 0), ("cross", 0), ("start_x", 1, 0, 3), ("pass_z", 0, 1),
    ("pass_z", 2, 1), ("pass", 2, 0), ("cross", 1), ("start_x", 1, 3, 4), ("finish", 0),
    ("pass", 1, 1), ("pass", 0, 1), ("pass", 2, 1), ("finish", 1),
)


def line_width_of(width):
    return width // 16 * 6 // 32 * 16


def cuts_of(width):
    step, last = width // 4, width - line_width_of(width)
    cuts = [(lo, min(lo + step, last)) for lo in range(0, last, step)]
    return (cuts[-1], *cuts[:-1])


def outer_step_kernel(
    group_total,
    steps_in,
    tokens_in,
    acts,
    cotangent,
    params_in,
    first_in,
    second_in,
    anchor_in,
    momentum_in,
    anchor_out,
    momentum_out,
    weights_out,
    steps_smem,
    tokens_smem,
    acts_buf,
    cot_buf,
    cot_t,
    own,
    far_z,
    x_send,
    x_recv,
    x_send_scale,
    x_recv_scale,
    z_send,
    z_send_scale,
    down_recv,
    down_scale,
    up_recv,
    up_scale,
    zz_send,
    zz_send_scale,
    down_z,
    down_z_scale,
    up_z,
    up_z_scale,
    cross_send,
    cross_recv,
    cross_send_scale,
    cross_recv_scale,
    params,
    first,
    second,
    anchor,
    momentum,
    weighted_send,
    weighted_recv,
    fresh_send,
    measure_buf,
    vouch_sem,
    acts_send_sem,
    acts_recv_sem,
    cot_sem,
    state_sem,
    x_send_sem,
    x_recv_sem,
    z_send_sem,
    down_sem,
    up_sem,
    zz_send_sem,
    down_z_sem,
    up_z_sem,
    cross_send_sem,
    cross_recv_sem,
    weighted_sem,
    fresh_sem,
):
    tokens, _ = acts.shape
    rows, width = params.shape
    half = rows // 2
    line_width = line_width_of(width)
    cuts = cuts_of(width)
    parts = len(cuts)
    tail = slice(width - line_width, width)
    me = lax.axis_index("fsdp")
    group = lax.axis_index("group")
    other_group = 1 - group
    core, x, z = me % 2, (me // 2) % 2, me // 4
    lower = z < 2
    corner = (z == 0) | (z == LINE - 1)
    middle = jnp.logical_not(corner)
    toward = jnp.where(lower, 1, -1)

    sibling = (group, me + 1 - 2 * core)
    across = (group, me + 2 - 4 * x)
    above = (group, me + 4 * toward)
    below = (group, me - 4 * toward)
    beyond = (group, me + 8 * toward)
    peer = (other_group, me)

    def place(n):
        mid = jnp.where(n == 0, 3, jnp.where(n == 1, 0, jnp.where(n == 2, 2, 1)))
        level = jnp.where(corner, 3 - n, mid)
        return jnp.where(lower, level, 3 - level)

    def half_of(i):
        return (other_group + i) % 2

    def columns(n, far, i, owner_core):
        owner_x = jnp.where(far == 1, 1 - x, x)
        block = (place(n) * 2 + owner_x) * 2 + owner_core
        return pl.ds(pl.multiple_of(block * rows + half_of(i) * half, half), half)

    def acts_local(n, i, far):
        return pltpu.make_async_copy(
            acts.at[:, columns(n, far, i, core)],
            acts_buf.at[i, n, far, pl.ds(0, tokens)],
            acts_recv_sem.at[i, n, far],
        )

    def acts_remote(n, i, far):
        return pltpu.make_async_remote_copy(
            src_ref=acts.at[:, columns(n, far, i, 1 - core)],
            dst_ref=acts_buf.at[i, n, far, pl.ds(tokens, tokens)],
            send_sem=acts_send_sem,
            recv_sem=acts_recv_sem.at[i, n, far],
            device_id=sibling,
            device_id_type=MESH,
        )

    def acts_arrived(n, i, far):
        whole = acts_buf.at[i, n, far]
        pltpu.make_async_copy(whole, whole, acts_recv_sem.at[i, n, far]).wait()

    def fetch(n, i):
        for far in (1, 0):
            acts_local(n, i, far).start()
            acts_remote(n, i, far).start()

    def remote(src, dst, send_sem, recv_sem, target):
        return pltpu.make_async_remote_copy(
            src_ref=src, dst_ref=dst, send_sem=send_sem, recv_sem=recv_sem, device_id=target, device_id_type=MESH
        )

    def x_copies(n, i, p):
        lo, hi = cuts[p]
        return (
            remote(
                x_send_scale.at[n, i, p], x_recv_scale.at[n, i, p],
                x_send_sem.at[0], x_recv_sem.at[n, i, p], across,
            ),
            remote(
                x_send.at[n, i, pl.ds(lo, hi - lo)], x_recv.at[n, i, pl.ds(lo, hi - lo)],
                x_send_sem.at[1], x_recv_sem.at[n, i, p], across,
            ),
        )

    def line_copies(n, i, p, into, scale, sem, slot, target):
        lo, hi = cuts[p]
        return (
            remote(
                z_send_scale.at[n, i, p], scale.at[slot, i, p],
                z_send_sem.at[0], sem.at[slot, i, p], target,
            ),
            remote(
                z_send.at[n, i, pl.ds(lo, hi - lo)], into.at[slot, i, pl.ds(lo, hi - lo)],
                z_send_sem.at[1], sem.at[slot, i, p], target,
            ),
        )

    def line_z_copies(n, i, into, scale, sem, slot, target):
        return (
            remote(
                zz_send_scale.at[n, i], scale.at[slot, i],
                zz_send_sem.at[0], sem.at[slot, i], target,
            ),
            remote(
                zz_send.at[n, i], into.at[slot, i],
                zz_send_sem.at[1], sem.at[slot, i], target,
            ),
        )

    def corner_send(n, i, p):
        return line_copies(n, i, p, down_recv, down_scale, down_sem, n, above)

    def middle_send(n, i, p):
        slot, target = MIDDLE_ROUTE[n]
        return line_copies(n, i, p, up_recv, up_scale, up_sem, slot, (beyond, below, above)[target])

    def corner_send_z(n, i):
        return line_z_copies(n, i, down_z, down_z_scale, down_z_sem, n, above)

    def middle_send_z(n, i):
        slot, target = MIDDLE_ROUTE[n]
        return line_z_copies(n, i, up_z, up_z_scale, up_z_sem, slot, (beyond, below, above)[target])

    def cross_copies(i):
        return (
            remote(
                cross_send_scale.at[i], cross_recv_scale.at[i],
                cross_send_sem.at[0], cross_recv_sem.at[i], across,
            ),
            remote(
                cross_send.at[i], cross_recv.at[i],
                cross_send_sem.at[1], cross_recv_sem.at[i], across,
            ),
        )

    def lanes_of(h):
        return slice(cuts[h][0], cuts[h][1] if h > 0 else width)

    def weighted_copy(h):
        at = lanes_of(h)
        return remote(
            weighted_send.at[:, at], weighted_recv.at[:, at], weighted_sem.at[parts], weighted_sem.at[h], peer
        )

    def fresh_copy(h):
        at = lanes_of(h)
        mine = pl.ds(pl.multiple_of(group * half, half), half)
        return remote(fresh_send.at[:, at], weights_out.at[mine, at], fresh_sem.at[parts], fresh_sem.at[h], peer)

    def start(copies):
        for copy in copies:
            copy.start()

    def arrived(sem, coded_rows, scale_rows=1):
        both = measure_buf.at[pl.ds(0, coded_rows // 2 + scale_rows)]
        pltpu.make_async_copy(both, both, sem).wait()

    state = []
    for n, (src, dst) in enumerate(
        (
            (params_in, params), (first_in, first), (second_in, second), (anchor_in, anchor), (momentum_in, momentum),
            (steps_in, steps_smem), (tokens_in, tokens_smem),
        )
    ):
        state.append(pltpu.make_async_copy(src, dst, state_sem.at[n]))
    cot_local = pltpu.make_async_copy(cotangent, cot_buf.at[pl.ds(0, tokens)], cot_sem.at[0])
    cot_remote = pltpu.make_async_remote_copy(
        src_ref=cotangent,
        dst_ref=cot_buf.at[pl.ds(tokens, tokens)],
        send_sem=cot_sem.at[1],
        recv_sem=cot_sem.at[2],
        device_id=sibling,
        device_id_type=MESH,
    )

    barrier = pltpu.get_barrier_semaphore()
    for target in (sibling, across, above, peer):
        pl.semaphore_signal(barrier, inc=1, device_id=target, device_id_type=MESH)

    @pl.when(middle)
    def _():
        pl.semaphore_signal(barrier, inc=1, device_id=below, device_id_type=MESH)

    cot_local.start()
    for n in range(2):
        for far in (1, 0):
            acts_local(n, 0, far).start()
    pl.semaphore_wait(barrier, jnp.where(middle, 5, 4))
    cot_remote.start()
    for far in (1, 0):
        acts_remote(0, 0, far).start()
    for far in (1, 0):
        acts_remote(1, 0, far).start()

    @pl.when(middle)
    def _():
        pl.semaphore_signal(vouch_sem, inc=1, device_id=above, device_id_type=MESH)

    def encode(value):
        top = jnp.max(jnp.abs(value), axis=0, keepdims=True)
        levels = jnp.where(top > SMALLEST, LEVELS / jnp.maximum(top, SMALLEST), 0.0)
        return jnp.round(value * levels).astype(jnp.int32).astype(WIRE), top * (1.0 / LEVELS)

    def decode(coded, scale):
        return coded.astype(jnp.int32).astype(jnp.float32) * scale

    cot_local.wait()
    cot_t[:, 0:tokens] = cot_buf[0:tokens].astype(jnp.float32).T.astype(jnp.bfloat16)
    cot_remote.wait_recv()
    for n in range(2, LINE):
        fetch(n, 0)
    cot_t[:, tokens:] = cot_buf[tokens:].astype(jnp.float32).T.astype(jnp.bfloat16)

    def multiply(i):
        @pl.loop(0, LINE)
        def _(n):
            if i == 0:

                @pl.when(n >= LINE // 2)
                def _():
                    fetch(2 * n - LINE, 1)
                    fetch(2 * n - LINE + 1, 1)

            acts_arrived(n, i, 1)
            for p, (lo, hi) in enumerate(cuts):
                product = jnp.dot(cot_t[lanes_of(p)], acts_buf[i, n, 1], preferred_element_type=jnp.float32)
                x_send[n, i, lo:hi], x_send_scale[n, i, p] = encode(product[: hi - lo])
                if p == 0:
                    far_z[n, i] = product[hi - lo :]
            if i == 0:
                for p in range(parts):
                    start(x_copies(n, i, p))
            acts_arrived(n, i, 0)
            for p in range(parts):
                at = lanes_of(p)
                own[n, i, at] = jnp.dot(cot_t[at], acts_buf[i, n, 0], preferred_element_type=jnp.float32)

            @pl.when((corner & (n < LINE - 1)) | (middle & (n == 1)))
            def _():
                zz_send[n, i, 0], zz_send_scale[n, i, 0] = encode(own[n, i, tail])
                zz_send[n, i, 1], zz_send_scale[n, i, 1] = encode(far_z[n, i])

            @pl.when(corner & (n < LINE - 1))
            def _():
                start(corner_send_z(n, i))

            @pl.when(middle & (n == 1))
            def _():
                start(middle_send_z(1, i))

    def received(n, i, p):
        lo, hi = cuts[p]
        arrived(x_recv_sem.at[n, i, p], hi - lo)
        return own[n, i, lo:hi] + decode(x_recv[n, i, lo:hi], x_recv_scale[n, i, p])

    def plus_line(total, i, p, into, scale, sem, slot):
        lo, hi = cuts[p]
        arrived(sem.at[slot, i, p], hi - lo)
        return total + decode(into[slot, i, lo:hi], scale[slot, i, p])

    def plus_below(total, i, p, slot):
        return plus_line(total, i, p, down_recv, down_scale, down_sem, slot)

    def plus_above(total, i, p, slot):
        return plus_line(total, i, p, up_recv, up_scale, up_sem, slot)

    def hand_on(role, n, i, p):
        lo, hi = cuts[p]
        total = received(n, i, p)
        if role == "middle" and n != 1:
            total = plus_below(total, i, p, n // 2)
        z_send[n, i, lo:hi], z_send_scale[n, i, p] = encode(total)
        start(corner_send(n, i, p) if role == "corner" else middle_send(n, i, p))

    def line_z(n, i, above_slots, below_slots):
        streams = [(up_z, up_z_scale, up_z_sem, slot) for slot in above_slots]
        streams += [(down_z, down_z_scale, down_z_sem, slot) for slot in below_slots]
        totals = [own[n, i, tail], far_z[n, i]]
        for into, scale, sem, slot in streams:
            arrived(sem.at[slot, i], 2 * line_width, 2)
            totals = [totals[far] + decode(into[slot, i, far], scale[slot, i, far]) for far in range(2)]
        return totals

    def hand_on_z(n, i):
        totals = line_z(n, i, (), (n // 2,))
        for far in range(2):
            zz_send[n, i, far], zz_send_scale[n, i, far] = encode(totals[far])
        start(middle_send_z(n, i))

    def cross_over(role, i):
        totals = line_z(3, i, (0, 1), ()) if role == "corner" else line_z(3, i, (1,), (2,))
        cross_send[i], cross_send_scale[i] = encode(totals[1])
        start(cross_copies(i))
        own[3, i, tail] = totals[0]

    def correction(beta):
        count = jnp.full((1, 1), steps_smem[group], jnp.int32).astype(jnp.float32)
        return 1.0 - jnp.exp(count * float(np.log(np.float64(np.float32(beta)))))

    def share_of(at):
        return jnp.full((1, 1), tokens_smem[at], jnp.int32).astype(jnp.float32)

    def finish(role, i, h):
        total = received(3, i, h)
        if role == "corner":
            total = plus_above(total, i, h, 0)
            total = plus_above(total, i, h, 1)
        else:
            total = plus_above(total, i, h, 1)
            total = plus_below(total, i, h, 2)
        if h == 0:
            arrived(cross_recv_sem.at[i], line_width)
            total = jnp.concatenate([total, own[3, i, tail] + decode(cross_recv[i], cross_recv_scale[i])], axis=0)
        lanes = lanes_of(h)
        gradient = total.T / group_total
        at = pl.ds(pl.multiple_of(half_of(i) * half, half), half)
        weights = params[at, lanes]
        fresh_first = beta_one * first[at, lanes] + (1.0 - beta_one) * gradient
        fresh_second = beta_two * second[at, lanes] + (1.0 - beta_two) * gradient * gradient
        ratio = fresh_first / correction(beta_one) / (jnp.sqrt(fresh_second / correction(beta_two)) + epsilon)
        share = share_of(group) / (share_of(0) + share_of(1))
        weighted = share * (weights - inner_rate * (ratio + decay_rate * weights))
        if i == 0:
            weighted_send[:, lanes] = weighted
            weighted_copy(h).start()
            return
        weighted_copy(h).wait_recv()
        new_anchor, new_momentum = outer_update(anchor[:, lanes], momentum[:, lanes], weighted + weighted_recv[:, lanes])
        rounded = new_anchor.astype(jnp.bfloat16)
        fresh_send[:, lanes] = rounded
        fresh_copy(h).start()
        anchor_out[:, lanes] = new_anchor
        momentum_out[:, lanes] = new_momentum
        weights_out[at, lanes] = rounded

    def run(role, plan):
        for event in plan:
            kind, rest = event[0], event[1:]
            if kind == "pass":
                for p in range(parts):
                    hand_on(role, *rest, p)
            elif kind == "pass_z":
                hand_on_z(*rest)
            elif kind == "cross":
                cross_over(role, *rest)
            elif kind == "start_x":
                for n in range(*rest[1:]):
                    for p in range(parts):
                        start(x_copies(n, rest[0], p))
            else:
                for h in range(parts):
                    finish(role, *rest, h)

    multiply(0)
    for copy in state:
        copy.start()

    @pl.when(corner)
    def _():
        run("corner", (("pass", 0, 0),))

    @pl.when(middle)
    def _():
        pl.semaphore_wait(vouch_sem, 1)
        run("middle", (("pass_z", 0, 0),))

    multiply(1)
    for copy in state:
        copy.wait()

    @pl.when(corner)
    def _():
        run("corner", CORNER_PLAN)

    @pl.when(middle)
    def _():
        run("middle", MIDDLE_PLAN)

    for h in range(parts):
        fresh_copy(h).wait_recv()

    cot_remote.wait_send()
    remote(acts_buf.at[0], acts_buf.at[0], acts_send_sem, acts_send_sem, sibling).wait_send()
    for buffer, sem in (
        (x_send_scale, x_send_sem.at[0]),
        (x_send, x_send_sem.at[1]),
        (z_send_scale, z_send_sem.at[0]),
        (z_send, z_send_sem.at[1]),
        (zz_send_scale, zz_send_sem.at[0]),
        (zz_send, zz_send_sem.at[1]),
        (cross_send_scale, cross_send_sem.at[0]),
        (cross_send, cross_send_sem.at[1]),
        (weighted_send, weighted_sem.at[parts]),
        (fresh_send, fresh_sem.at[parts]),
    ):
        remote(buffer, buffer, sem, sem, sibling).wait_send()


def write_out_kernel(anchor, momentum, weights, anchor_out, momentum_out, weights_out, sem):
    copies = [
        pltpu.make_async_copy(src, dst, sem.at[n])
        for n, (src, dst) in enumerate(((anchor, anchor_out), (momentum, momentum_out), (weights, weights_out)))
    ]
    for copy in copies:
        copy.start()
    for copy in copies:
        copy.wait()


def fused_per_device(
    acts, cotangent, inner_params, adam_first, adam_second, inner_steps, group_tokens, anchor, momentum
):
    tokens, _ = acts.shape[1:]
    rows, width = inner_params.shape[1:]
    half, line_width = rows // 2, line_width_of(width)
    low, full = jnp.bfloat16, jnp.float32
    dma = pltpu.SemaphoreType.DMA
    vmem = pltpu.VMEM
    body = width - line_width
    parts = len(cuts_of(width))
    operands = (
        inner_steps, group_tokens, acts[0], cotangent[0], inner_params[0], adam_first[0], adam_second[0],
        anchor, momentum,
    )
    results = pl.pallas_call(
        functools.partial(outer_step_kernel, tokens * lax.axis_size("fsdp")),
        out_shape=(
            vmem(anchor.shape, full),
            vmem(anchor.shape, full),
            vmem((rows, width), low),
        ),
        in_specs=[pl.BlockSpec(memory_space=pltpu.HBM)] * 9,
        out_specs=[pl.BlockSpec(memory_space=pltpu.VMEM)] * 3,
        scratch_shapes=[
            pltpu.SMEM(inner_steps.shape, jnp.int32),
            pltpu.SMEM(group_tokens.shape, jnp.int32),
            vmem((2, LINE, 2, 2 * tokens, half), low),
            vmem((2 * tokens, width), low),
            vmem((width, 2 * tokens), low),
            vmem((LINE, 2, width, half), full),
            vmem((LINE, 2, line_width, half), full),
            vmem((LINE, 2, body, half), WIRE),
            vmem((LINE, 2, body, half), WIRE),
            vmem((LINE, 2, parts, 1, half), full),
            vmem((LINE, 2, parts, 1, half), full),
            vmem((3, 2, body, half), WIRE),
            vmem((3, 2, parts, 1, half), full),
            vmem((3, 2, body, half), WIRE),
            vmem((3, 2, parts, 1, half), full),
            vmem((2, 2, body, half), WIRE),
            vmem((2, 2, parts, 1, half), full),
            vmem((3, 2, 2, line_width, half), WIRE),
            vmem((3, 2, 2, 1, half), full),
            vmem((3, 2, 2, line_width, half), WIRE),
            vmem((3, 2, 2, 1, half), full),
            vmem((2, 2, 2, line_width, half), WIRE),
            vmem((2, 2, 2, 1, half), full),
            vmem((2, line_width, half), WIRE),
            vmem((2, line_width, half), WIRE),
            vmem((2, 1, half), full),
            vmem((2, 1, half), full),
            *[vmem((rows, width), full)] * 3,
            *[vmem((half, width), full)] * 2,
            *[vmem((half, width), full)] * 2,
            vmem((half, width), low),
            vmem((max(width // 8, line_width) + 2, 1, half), full),
            pltpu.SemaphoreType.REGULAR,
            dma,
            dma((2, LINE, 2)),
            dma((3,)),
            dma((7,)),
            dma((2,)),
            dma((LINE, 2, parts)),
            dma((2,)),
            dma((3, 2, parts)),
            dma((2, 2, parts)),
            dma((2,)),
            dma((3, 2)),
            dma((2, 2)),
            dma((2,)),
            dma((2,)),
            dma((parts + 1,)),
            dma((parts + 1,)),
        ],
        compiler_params=pltpu.CompilerParams(
            collective_id=0, has_side_effects=True, vmem_limit_bytes=48 * 1024 * 1024
        ),
    )(*(pltpu.with_memory_space_constraint(operand, pltpu.HBM) for operand in operands))
    new_anchor, new_momentum, weights = pl.pallas_call(
        write_out_kernel,
        out_shape=(
            jax.ShapeDtypeStruct(anchor.shape, full),
            jax.ShapeDtypeStruct(anchor.shape, full),
            jax.ShapeDtypeStruct((rows, width), low),
        ),
        in_specs=[pl.BlockSpec(memory_space=pltpu.VMEM)] * 3,
        out_specs=[pl.BlockSpec(memory_space=pl.ANY)] * 3,
        scratch_shapes=[dma((3,))],
        compiler_params=pltpu.CompilerParams(vmem_limit_bytes=4 * 1024 * 1024),
    )(*results)
    return (new_anchor, new_momentum, weights[None])


def choose(*arguments):
    rows, width = arguments[2].shape[1:]
    fits = lax.axis_size("fsdp") == FSDP and lax.axis_size("group") == GROUPS
    if fits and rows % 256 == 0 and width % 512 == 0:
        return fused_per_device(*arguments)
    return per_device(*arguments)


def solution(mesh):
    placed = (
        P("group", "fsdp", None),
        P("group", "fsdp", None),
        P("group", "fsdp", None),
        P("group", "fsdp", None),
        P("group", "fsdp", None),
        P(),
        P(),
        P(("fsdp", "group"), None),
        P(("fsdp", "group"), None),
    )
    return jax.shard_map(
        choose,
        mesh=mesh,
        in_specs=placed,
        out_specs=(
            P(("fsdp", "group"), None),
            P(("fsdp", "group"), None),
            P("group", "fsdp", None),
        ),
        check_vma=False,
    )
```
